256 devices in a mesh: lat: 8 (over z), lon: 16 (over x, y), obs: 2 (over core).
Axes of the slice: x: 4, y: 4, z: 8, core: 2. Of those that a mesh axis runs over, the one named last changes fastest.
Arguments:
- innovation: float32 [32768, 128], P(('lat', 'lon', 'obs')), may hold values from -6 to 6
- obs_error: float32 [32768, 128], P(('lat', 'lon', 'obs')), may hold values from 0.5 to 2
- obs_offset: float32 [2, 32768, 128], P(None, ('lat', 'lon', 'obs')), may hold values from 0 to 1
- obs_cell: int32 [32768, 128], P(('lat', 'lon', 'obs')), may hold values from 0 to 65535
- obs_owner: int32 [256, 128], P(('lat', 'lon', 'obs')), may hold values from 0 to 127, as said below
- block_count: int32 [256], P(('lat', 'lon', 'obs')), may hold values from 64 to 128
- land_mask: int32 [512, 16384], P(('lat', 'obs'), 'lon'), may hold values from 0 to 1, as said below
- inertia: float32 [512, 16384], P(('lat', 'obs'), 'lon'), may hold values from 0.002 to 0.05
- sea_depth: float32 [512, 16384], P(('lat', 'obs'), 'lon'), may hold values from 0.5 to 5
Outputs:
- adjoint_field: float32 [512, 16384], P(('lat', 'obs'), 'lon')
- residual: float32 [512, 16384], P(('lat', 'obs'), 'lon')
The draws below stay inside these ranges and needn't reach their ends.
Inputs may be any that keep to these rules, and one draw needn't show every extreme that they name: `obs_owner`: among the live blocks of one device at most 3 name the same tile; in every draw some tile is named by exactly 3 live blocks of every device. `land_mask`: the first and the last grid row are land.
All inputs are finite; a program needn't handle non-finite values.
Results may differ from the reference program's by a relative error of at most 0.0003.
Values sent between devices are 32-bit elements; how exact they have to be, the bound alone decides.
A program may use at most 64 MiB of HBM per device.

```python
import math
import jax
import jax.numpy as jnp

TILE_R = 64
TILE_C = 1024
NBLK = 128
BLOCK = 128
ITERS = 5
CAPB = 3
NLAT = 512
NLON = 16384
N_LAT = 8
N_LON = 16
DEVICES = 256


def owner_plan(key):
    tile_count = N_LAT * N_LON
    slot_total = tile_count * CAPB
    base_key = jax.random.fold_in(key, 7711)
    block_counts = jax.random.randint(jax.random.fold_in(base_key, 1), (DEVICES,), NBLK // 2, NBLK + 1)
    hot_tile = jax.random.randint(jax.random.fold_in(base_key, 2), (), 0, tile_count)
    device_keys = jax.random.split(jax.random.fold_in(base_key, 3), DEVICES)

    def device_plan(dev_key, live_total):
        perm_key, mix_key = jax.random.split(dev_key)
        shuffled = jax.random.permutation(perm_key, slot_total)
        slot_ids = jnp.arange(slot_total)
        is_hot = slot_ids // CAPB == hot_tile
        sort_key = jnp.where(is_hot, slot_ids - slot_total, shuffled)
        chosen = jnp.argsort(sort_key)[:NBLK]
        owners = chosen // CAPB
        block_ids = jnp.arange(NBLK)
        mixing = jax.random.permutation(mix_key, NBLK)
        live_key = jnp.where(block_ids < live_total, mixing, NBLK + block_ids)
        return owners[jnp.argsort(live_key)]
    owners = jax.vmap(device_plan)(device_keys, block_counts)
    return (block_counts.astype(jnp.int32), owners.astype(jnp.int32))


def draw_obs_owner(key, part):
    return owner_plan(key)[1]


def draw_block_count(key, part):
    return owner_plan(key)[0]


def draw_land_mask(key, part):
    land_bits = jax.random.randint(jax.random.fold_in(key, 913), (NLAT, NLON), 0, 10)
    row_ids = jnp.arange(NLAT)[:, None]
    ocean = (land_bits < 7) & (row_ids > 0) & (row_ids < NLAT - 1)
    return ocean.astype(jnp.int32)


def touch_ends(result, rng, smallest, top_value):
    shape = result.shape
    index_at = [jax.random.randint(jax.random.fold_in(rng, axis), (), 0, shape[axis]) for axis in range(len(shape))]
    result = result.at[tuple(index_at)].set(smallest)
    longest = shape.index(max(shape))
    index_at[longest] = (index_at[longest] + 1) % shape[longest]
    return result.at[tuple(index_at)].set(top_value)


def block_levels(own_key, extent, cuts, smallest, high):
    level, own = 1.0, jax.random.fold_in(own_key, 6)
    for axis_at, blocks in cuts:
        steps = jnp.exp(jax.random.uniform(jax.random.fold_in(own, axis_at), (blocks,), jnp.float32, smallest / len(cuts), high / len(cuts)))
        level = level * jnp.repeat(steps, extent[axis_at] // blocks).reshape([-1 if axis == axis_at else 1 for axis in range(len(extent))])
    return level


def bell_draw(key, shape, deviation, limit, cuts=(), held_as=jnp.bfloat16):
    gain = block_levels(key, shape, cuts, -0.22, 0.18) if cuts else 1.0
    array = jax.random.normal(key, shape, jnp.float32) * deviation * gain
    return jnp.minimum(jnp.maximum(array, -limit), limit).astype(held_as)


def setup_inputs(seed: int = 0) -> dict:
    splits = jax.random.split(jax.random.key(seed), 10)
    return {
        "innovation": bell_draw(splits[0], (DEVICES * NBLK, BLOCK), 1.0, 6.0, ((0, 256),), jnp.float32),
        "obs_error": jnp.clip(jnp.exp(math.log(2.0) - 1.3862944 * jax.random.uniform(splits[1], (DEVICES * NBLK, BLOCK), jnp.float32) ** block_levels(splits[1], (DEVICES * NBLK, BLOCK), ((0, 256),), -0.2, 0.2)), 0.5, 2.0),
        "obs_offset": jnp.clip(1.0 * jax.random.uniform(splits[2], (2, DEVICES * NBLK, BLOCK), jnp.float32) ** block_levels(splits[2], (2, DEVICES * NBLK, BLOCK), ((1, 256),), -0.2, 0.2), 0.0, 1.0),
        "obs_cell": touch_ends(jax.random.randint(splits[3], (DEVICES * NBLK, BLOCK), 0, TILE_R * TILE_C), jax.random.fold_in(splits[3], 1), 0, (TILE_R * TILE_C) - 1).astype(jnp.int32),
        "obs_owner": draw_obs_owner(jax.random.fold_in(splits[9], 71), 0),
        "block_count": draw_block_count(jax.random.fold_in(splits[9], 71), 0),
        "land_mask": draw_land_mask(jax.random.fold_in(splits[9], 71), 0),
        "inertia": jnp.clip(jnp.exp(math.log(0.05) - 3.218876 * jax.random.uniform(splits[7], (NLAT, NLON), jnp.float32) ** block_levels(splits[7], (NLAT, NLON), ((0, 16), (1, 16)), -0.2, 0.2)), 0.002, 0.05),
        "sea_depth": jnp.clip(jnp.exp(math.log(5.0) - 2.3025851 * jax.random.uniform(splits[8], (NLAT, NLON), jnp.float32) ** block_levels(splits[8], (NLAT, NLON), ((0, 16), (1, 16)), -0.2, 0.2)), 0.5, 5.0),
    }


def reference(innovation, obs_error, obs_offset, obs_cell, obs_owner, block_count, land_mask, inertia, sea_depth):
    is_live = (jnp.arange(NBLK)[None, :] < block_count[:, None]).reshape(-1)
    owner_tile = obs_owner.reshape(-1)
    scaled = jnp.where(is_live[:, None], innovation / (obs_error * obs_error), jnp.float32(0.0))
    north_frac = obs_offset[0]
    east_frac = obs_offset[1]
    cell_row = (owner_tile // N_LON)[:, None] * TILE_R + obs_cell // TILE_C
    cell_col = (owner_tile % N_LON)[:, None] * TILE_C + obs_cell % TILE_C
    next_col = (cell_col + 1) % NLON
    next_row = cell_row + 1
    cell_total = NLAT * NLON
    inside = next_row < NLAT
    segment_ids = jnp.concatenate([(cell_row * NLON + cell_col).reshape(-1), (cell_row * NLON + next_col).reshape(-1), jnp.where(inside, next_row * NLON + cell_col, cell_total).reshape(-1), jnp.where(inside, next_row * NLON + next_col, cell_total).reshape(-1)]).astype(jnp.int32)
    contribs = jnp.concatenate([(scaled * ((1.0 - north_frac) * (1.0 - east_frac))).reshape(-1), (scaled * ((1.0 - north_frac) * east_frac)).reshape(-1), (scaled * (north_frac * (1.0 - east_frac))).reshape(-1), (scaled * (north_frac * east_frac)).reshape(-1)])
    partial_value = jax.ops.segment_sum(contribs, segment_ids, num_segments=cell_total + 1)[:cell_total]
    ocean = land_mask.astype(jnp.float32)
    forcing = partial_value.reshape(NLAT, NLON) * ocean
    conduct = ocean * sea_depth
    cond_north = jnp.sqrt(conduct * jnp.roll(conduct, 1, 0))
    cond_south = jnp.sqrt(conduct * jnp.roll(conduct, -1, 0))
    cond_west = jnp.sqrt(conduct * jnp.roll(conduct, 1, 1))
    cond_east = jnp.sqrt(conduct * jnp.roll(conduct, -1, 1))
    diagonal = inertia + cond_north + cond_south + cond_west + cond_east

    def operate(field):
        return diagonal * field - cond_north * jnp.roll(field, 1, 0) - cond_south * jnp.roll(field, -1, 0) - cond_west * jnp.roll(field, 1, 1) - cond_east * jnp.roll(field, -1, 1)
    adjoint_field = jnp.zeros_like(forcing)
    residual = forcing
    direction = forcing
    norm_now = jnp.sum(residual * residual)
    for iteration in range(ITERS):
        applied = operate(direction)
        step_size = norm_now / jnp.sum(direction * applied)
        adjoint_field = adjoint_field + step_size * direction
        residual = residual - step_size * applied
        norm_next = jnp.sum(residual * residual)
        direction = residual + norm_next / norm_now * direction
        norm_now = norm_next
    return (adjoint_field, residual)
```

```python
import functools

import jax
import jax.numpy as jnp
from jax import lax
from jax.experimental import pallas as pl
from jax.experimental.pallas import tpu as pltpu
from jax.sharding import PartitionSpec as P

ITERS = 5
CAP = 3
FIELDS = 4
ROWS = CAP * FIELDS
SPLIT = 4
PART = SPLIT + 1
LANE = 128
EDGE = 8
F32 = jnp.float32
BF16 = jnp.bfloat16
MESH = pl.DeviceIdType.MESH
CENTRE = 9.0
RADIUS = 9.0
TRUST = 1000.0


def iota(shape, dim):
    return lax.broadcasted_iota(jnp.int32, shape, dim)


def arrange(tiles, innovation, error, offset, cell, owner, count, send):
    blocks = innovation.shape[0]
    slots = tiles * CAP
    owners = owner[...]
    live = count[0]
    row, col = iota((blocks, blocks), 0), iota((blocks, blocks), 1)
    owners_f = owners.astype(F32)
    owners_col = jnp.sum(jnp.where(row == col, owners_f, 0.0), axis=1, keepdims=True)
    earlier = (owners_col == owners_f) & (row < col) & (row < live)
    rank = jnp.sum(jnp.where(earlier, 1.0, 0.0), axis=0, keepdims=True)
    lane = iota((1, blocks), 1)
    target = jnp.where(lane < live, owners_f * CAP + rank, -1.0)
    pick = jnp.where(iota((slots, blocks), 0).astype(F32) == target, 1.0, 0.0).astype(BF16)
    err = error[...]
    rest = jnp.concatenate(
        [innovation[...] / (err * err), offset[0], offset[1], cell[...].astype(F32)], axis=1
    )
    out = None
    for _ in range(3):
        part = rest.astype(BF16)
        term = jnp.dot(pick, part, preferred_element_type=F32)
        out = term if out is None else out + term
        rest = rest - part.astype(F32)
    for f in range(FIELDS):
        send[pl.ds(f, slots, stride=FIELDS), :] = out[:, f * LANE : (f + 1) * LANE]


def weights_of(values, rows, cols):
    amount, north, east = values[0:1], values[1:2], values[2:3]
    cell = values[3:4].astype(jnp.int32)
    cell_row = cell // cols
    cell_col = cell % cols
    part = cell_col % SPLIT
    spot = iota((8, LANE), 0)
    across = jnp.where(spot == part, 1.0 - east, jnp.where(spot == part + 1, east, 0.0)) * amount
    down_at = iota((rows, LANE), 0)
    down = jnp.where(down_at == cell_row, 1.0 - north, jnp.where(down_at == cell_row + 1, north, 0.0))
    below = jnp.where(cell_row == rows - 1, north, 0.0) * across
    pieces = [down * across[c : c + 1] for c in range(PART)]
    pieces += [below, jnp.zeros((8, LANE), F32)]
    weight = jnp.concatenate(pieces, axis=0)
    hot = jnp.where(iota((cols // SPLIT, LANE), 0) == cell_col // SPLIT, 1.0, 0.0).astype(BF16)
    return weight, hot


def spread_some(values, rows, cols, total):
    sides = [weights_of(values[i : i + FIELDS], rows, cols) for i in range(0, values.shape[0], FIELDS)]
    weight = jnp.concatenate([s[0] for s in sides], axis=1)
    hot = jnp.concatenate([s[1] for s in sides], axis=1)
    high = weight.astype(BF16)
    low = (weight - high.astype(F32)).astype(BF16)
    both = jnp.concatenate([high, low], axis=0)
    total[...] += lax.dot_general(both, hot, (((1,), (1,)), ((), ())), preferred_element_type=F32)


def total_shape(rows, cols):
    return (2 * (PART * rows + 16), cols // SPLIT)


def unpack(total, rows, cols, part):
    wide = cols // SPLIT
    half = rows // 2
    count = PART * rows + 16
    acc = total[0:count, :] + total[count : 2 * count, :]
    under = acc[PART * rows : PART * rows + 8]
    top = iota((8, wide), 0) == 0
    fields = []
    for c in range(PART):
        row = jnp.where(top, jnp.broadcast_to(under[c : c + 1], (8, wide)), 0.0)
        fields.append(jnp.concatenate([acc[c * rows : (c + 1) * rows], row], axis=0))
    carried = pltpu.roll(fields[SPLIT], 1, 1)
    first = iota(carried.shape, 1) == 0
    past = jnp.where(first, carried, 0.0)[:, :LANE]
    fields[0] = fields[0] + jnp.where(first, 0.0, carried)
    size = SPLIT * LANE
    source, place = iota((size, size), 0), iota((size, size), 1)
    order = jnp.where(place == SPLIT * (source % LANE) + source // LANE, 1.0, 0.0).astype(BF16)
    strips = []
    for j in range(wide // LANE):
        rest = jnp.concatenate([f[:, j * LANE : (j + 1) * LANE] for f in fields[:SPLIT]], axis=1)
        out = None
        for _ in range(3):
            piece = rest.astype(BF16)
            term = jnp.dot(piece, order, preferred_element_type=F32)
            out = term if out is None else out + term
            rest = rest - piece.astype(F32)
        strips.append(out)
    for j, out in enumerate(strips):
        at = slice(j * size, (j + 1) * size)
        part[0, 0:half, at] = out[0:half]
        part[0, half : half + 8, at] = jnp.zeros((8, size), F32)
        part[1, :, at] = out[half:]
    part[0, 0:half, cols:] = past[0:half]
    part[0, half : half + 8, cols:] = jnp.zeros((8, LANE), F32)
    part[1, :, cols:] = past[half:]


def spread_kernel(rows, cols, recv, part, total):
    total[...] = jnp.zeros_like(total)
    step = 2 * ROWS

    def some(i, carry):
        spread_some(recv[pl.ds(pl.multiple_of(i * step, 8), step), :], rows, cols, total)
        return carry

    lax.fori_loop(0, recv.shape[0] // step, some, 0)
    unpack(total, rows, cols, part)


def add_up(values):
    while len(values) > 1:
        rest = values[len(values) & ~1 :]
        values = [values[i] + values[i + 1] for i in range(0, len(values) - 1, 2)] + rest
    return values[0]


def coefficients(mu):
    start = mu[0]
    mu = [m / start for m in mu]
    gram = {}
    for s in range(2 * ITERS + 1):
        for d in range(s + 1):
            gram[s, d] = 0.5 * (mu[s] + mu[d])

    def inner(a, b):
        terms = [a[i] * b[j] * gram[i + j, abs(i - j)] for i in range(len(a)) for j in range(len(b))]
        return add_up(terms)

    def operate(a):
        out = [CENTRE * v for v in a] + [None]
        for i, v in enumerate(a):
            for j, f in ((1, RADIUS),) if i == 0 else ((i + 1, RADIUS / 2), (i - 1, RADIUS / 2)):
                out[j] = f * v if out[j] is None else out[j] + f * v
        return out

    one = jnp.ones_like(start)
    field, residual, direction = [], [one], [one]
    norm = one
    worst = one
    for _ in range(ITERS):
        applied = operate(direction)
        step = norm / inner(direction, applied)
        field = [
            step * d + (field[i] if i < len(field) else 0.0) for i, d in enumerate(direction)
        ]
        residual = [
            (residual[i] if i < len(residual) else 0.0) - step * a for i, a in enumerate(applied)
        ]
        after = inner(residual, residual)
        size = add_up([jnp.abs(v) for v in residual])
        worst = jnp.maximum(worst, jnp.where(after > 0, size * size / after, 1e30))
        ratio = after / norm
        direction = [
            v + (ratio * direction[i] if i < len(direction) else 0.0) for i, v in enumerate(residual)
        ]
        norm = after
    sound = jnp.where(worst < TRUST, 1.0, 0.0)
    return field, residual, sound


def solve_kernel(
    n_lat,
    n_lon,
    part,
    land,
    inertia,
    depth,
    field_out,
    residual_out,
    forcing_out,
    sound_out,
    got,
    mine,
    west,
    east,
    tall,
    above,
    below,
    coef,
    cond,
    basis,
    line_in,
    line_at,
    rank_in,
    rank_at,
    send_sem,
    recv_sem,
    line_send,
    line_recv,
    rank_send,
    rank_recv,
):
    rows, cols = land.shape
    high, wide = rows + 2 * EDGE, cols + 2 * LANE
    lat, lon, obs = lax.axis_index("lat"), lax.axis_index("lon"), lax.axis_index("obs")
    ranks = 2 * n_lat
    rank = lat * 2 + obs

    def on_line(k):
        return {"lon": k}

    def on_rank(k):
        return {"lat": k // 2, "obs": k % 2}

    barrier = pltpu.get_barrier_semaphore()

    def greet_line(d, carry):
        pl.semaphore_signal(barrier, 1, device_id=on_line((lon + d) % n_lon), device_id_type=MESH)
        return carry

    def greet_rank(d, carry):
        pl.semaphore_signal(barrier, 1, device_id=on_rank((rank + d) % ranks), device_id_type=MESH)
        return carry

    lax.fori_loop(1, n_lon, greet_line, 0)
    lax.fori_loop(1, ranks, greet_rank, 0)

    inner_rows, inner_cols = slice(EDGE, EDGE + rows), slice(LANE, LANE + cols)
    coef[0, inner_rows, inner_cols] = land[...].astype(F32) * depth[...]
    coef[1, inner_rows, inner_cols] = inertia[...]
    pl.semaphore_wait(barrier, n_lon - 1 + ranks - 1)

    def copy(k, src, dst, device):
        c = pltpu.make_async_remote_copy(
            src_ref=src,
            dst_ref=dst,
            send_sem=send_sem.at[k],
            recv_sem=recv_sem.at[k],
            device_id=device,
            device_id_type=MESH,
        )
        c.start()
        return c

    to_east, to_west = on_line((lon + 1) % n_lon), on_line((lon + n_lon - 1) % n_lon)
    to_south, to_north = on_rank((rank + 1) % ranks), on_rank((rank + ranks - 1) % ranks)
    own = pl.ds(EDGE, rows)

    pair = copy(0, part.at[1 - obs], got, {"obs": 1 - obs})
    coef_e = copy(1, coef.at[:, own, pl.ds(cols, LANE)], coef.at[:, own, pl.ds(0, LANE)], to_east)
    coef_w = copy(2, coef.at[:, own, pl.ds(LANE, LANE)], coef.at[:, own, pl.ds(LANE + cols, LANE)], to_west)
    pair.wait_recv()
    mine[...] = part[obs] + got[...]
    mine_e = copy(3, mine.at[:, pl.ds(cols - LANE, 2 * LANE)], west, to_east)
    mine_w = copy(4, mine.at[:, pl.ds(0, LANE)], east, to_west)
    coef_e.wait_recv()
    coef_w.wait_recv()
    coef_s = copy(5, coef.at[:, pl.ds(rows, EDGE), :], coef.at[:, pl.ds(0, EDGE), :], to_south)
    coef_n = copy(6, coef.at[:, pl.ds(EDGE, EDGE), :], coef.at[:, pl.ds(EDGE + rows, EDGE), :], to_north)
    mine_e.wait_recv()
    mine_w.wait_recv()
    tall[:, 0:LANE] = west[:, 0:LANE]
    tall[:, LANE : 2 * LANE] = mine[:, 0:LANE] + west[:, LANE:]
    tall[:, 2 * LANE : LANE + cols] = mine[:, LANE:cols]
    tall[:, LANE + cols :] = mine[:, cols:] + east[...]
    tall_s = copy(7, tall.at[pl.ds(rows - EDGE, 2 * EDGE), :], above, to_south)
    tall_n = copy(8, tall.at[pl.ds(0, EDGE), :], below, to_north)
    coef_s.wait_recv()
    coef_n.wait_recv()
    conduct = coef[0]
    north = jnp.sqrt(conduct * pltpu.roll(conduct, 1, 0))
    south = pltpu.roll(north, high - 1, 0)
    left = jnp.sqrt(conduct * pltpu.roll(conduct, 1, 1))
    right = pltpu.roll(left, wide - 1, 1)
    cond[0] = (coef[1] + north + south + left + right - CENTRE) * (1.0 / RADIUS)
    cond[1] = north * (1.0 / RADIUS)
    cond[2] = south * (1.0 / RADIUS)
    cond[3] = left * (1.0 / RADIUS)
    cond[4] = right * (1.0 / RADIUS)
    tall_s.wait_recv()
    tall_n.wait_recv()
    ocean = coef[0] > 0
    raw = jnp.concatenate(
        [
            above[0:EDGE, :],
            tall[0:EDGE, :] + above[EDGE:, :],
            tall[EDGE:rows, :],
            below[...] + tall[rows:, :],
        ],
        axis=0,
    )
    basis[0] = jnp.where(ocean, raw, 0.0)
    forcing_out[...] = basis[0, inner_rows, inner_cols]

    def operate(v):
        return (
            cond[0] * v
            - cond[1] * pltpu.roll(v, 1, 0)
            - cond[2] * pltpu.roll(v, high - 1, 0)
            - cond[3] * pltpu.roll(v, 1, 1)
            - cond[4] * pltpu.roll(v, wide - 1, 1)
        )

    for k in range(ITERS):
        after = operate(basis[k])
        basis[k + 1] = after if k == 0 else 2.0 * after - basis[k - 1]

    def dot(i, j):
        pieces = []
        for a in range(EDGE, EDGE + rows, 8):
            for b in range(LANE, LANE + cols, LANE):
                pieces.append(basis[i, a : a + 8, b : b + LANE] * basis[j, a : a + 8, b : b + LANE])
        return jnp.sum(add_up(pieces), axis=0, keepdims=True)

    pairs = [(k // 2, (k + 1) // 2) for k in range(2 * ITERS + 1)]
    sums = [dot(i, j) for i, j in pairs]
    stack = jnp.concatenate(sums + [jnp.zeros((16 - len(sums), LANE), F32)], axis=0)
    column = jnp.sum(stack, axis=1, keepdims=True)
    diag = iota((16, LANE), 0) == iota((16, LANE), 1)
    line_in[...] = jnp.sum(jnp.where(diag, column, 0.0), axis=0, keepdims=True)

    def share(count, me, device, value, at, s_sem, r_sem):
        def copy_of(slot, k, target):
            return pltpu.make_async_remote_copy(
                src_ref=value,
                dst_ref=at.at[slot],
                send_sem=s_sem.at[k],
                recv_sem=r_sem.at[slot],
                device_id=device(target),
                device_id_type=MESH,
            )

        def begin(d, carry):
            copy_of(me, d, (me + d) % count).start()
            return carry

        def arrive(d, carry):
            copy_of((me + count - d) % count, d, (me + d) % count).wait_recv()
            return carry

        def leave(d, carry):
            copy_of(me, d, (me + d) % count).wait_send()
            return carry

        lax.fori_loop(1, count, begin, 0)
        at[me] = value[...]
        lax.fori_loop(1, count, arrive, 0)
        lax.fori_loop(1, count, leave, 0)
        return add_up([at[k] for k in range(count)])

    rank_in[...] = share(n_lon, lon, on_line, line_in, line_at, line_send, line_recv)
    sums = share(ranks, rank, on_rank, rank_in, rank_at, rank_send, rank_recv)
    lane = iota((1, LANE), 1)
    raw_sums = [
        jnp.sum(jnp.where(lane == k, sums, 0.0), axis=1, keepdims=True) for k in range(2 * ITERS + 1)
    ]
    mu = [
        raw_sums[k] if k < 2 else 2.0 * raw_sums[k] - raw_sums[k % 2] for k in range(2 * ITERS + 1)
    ]
    field, residual, sound = coefficients(mu)
    views = [basis[k, inner_rows, inner_cols] for k in range(ITERS + 1)]
    field_out[...] = add_up([c * v for c, v in zip(field, views)])
    residual_out[...] = add_up([c * v for c, v in zip(residual, views)])
    sound_out[...] = jnp.broadcast_to(sound, (1, LANE))
    for c in (pair, coef_e, coef_w, mine_e, mine_w, coef_s, coef_n, tall_s, tall_n):
        c.wait_send()


def solve(n_lat, n_lon, part, land, inertia, depth):
    rows, cols = land.shape
    high, wide = rows + 2 * EDGE, cols + 2 * LANE
    own = jax.ShapeDtypeStruct((rows, cols), F32)
    vmem = pl.BlockSpec(memory_space=pltpu.VMEM)
    ranks = 2 * n_lat
    return pl.pallas_call(
        functools.partial(solve_kernel, n_lat, n_lon),
        out_shape=(own, own, own, jax.ShapeDtypeStruct((1, LANE), F32)),
        in_specs=[vmem] * 4,
        out_specs=(vmem,) * 4,
        scratch_shapes=[
            pltpu.VMEM((rows + EDGE, cols + LANE), F32),
            pltpu.VMEM((rows + EDGE, cols + LANE), F32),
            pltpu.VMEM((rows + EDGE, 2 * LANE), F32),
            pltpu.VMEM((rows + EDGE, LANE), F32),
            pltpu.VMEM((rows + EDGE, wide), F32),
            pltpu.VMEM((2 * EDGE, wide), F32),
            pltpu.VMEM((EDGE, wide), F32),
            pltpu.VMEM((2, high, wide), F32),
            pltpu.VMEM((5, high, wide), F32),
            pltpu.VMEM((ITERS + 1, high, wide), F32),
            pltpu.VMEM((1, LANE), F32),
            pltpu.VMEM((n_lon, 1, LANE), F32),
            pltpu.VMEM((1, LANE), F32),
            pltpu.VMEM((ranks, 1, LANE), F32),
            pltpu.SemaphoreType.DMA((9,)),
            pltpu.SemaphoreType.DMA((9,)),
            pltpu.SemaphoreType.DMA((n_lon,)),
            pltpu.SemaphoreType.DMA((n_lon,)),
            pltpu.SemaphoreType.DMA((ranks,)),
            pltpu.SemaphoreType.DMA((ranks,)),
        ],
        compiler_params=pltpu.CompilerParams(collective_id=1, has_side_effects=True),
    )(part, land, inertia, depth)


def shifted(value, axis, steps):
    count = lax.axis_size(axis)
    return lax.ppermute(value, axis, [(i, (i + steps) % count) for i in range(count)])


def border(block):
    for axis, dim in ((("lat", "obs"), 0), ("lon", 1)):
        size = block.shape[dim]
        low = shifted(lax.slice_in_dim(block, size - 1, size, axis=dim), axis, 1)
        high = shifted(lax.slice_in_dim(block, 0, 1, axis=dim), axis, -1)
        block = jnp.concatenate([low, block, high], axis=dim)
    return block


def stepwise(forcing, land, inertia, depth):
    conduct = land.astype(F32) * depth
    padded = border(conduct)
    north = jnp.sqrt(conduct * padded[:-2, 1:-1])
    south = jnp.sqrt(conduct * padded[2:, 1:-1])
    west = jnp.sqrt(conduct * padded[1:-1, :-2])
    east = jnp.sqrt(conduct * padded[1:-1, 2:])
    diagonal = inertia + north + south + west + east

    def whole(value):
        return lax.psum(jnp.sum(value), ("lat", "lon", "obs"))

    def step(_, state):
        field, residual, direction, norm = state
        outer = border(direction)
        applied = (
            diagonal * direction
            - north * outer[:-2, 1:-1]
            - south * outer[2:, 1:-1]
            - west * outer[1:-1, :-2]
            - east * outer[1:-1, 2:]
        )
        size = norm / whole(direction * applied)
        field = field + size * direction
        residual = residual - size * applied
        after = whole(residual * residual)
        return field, residual, residual + after / norm * direction, after

    state = (jnp.zeros_like(forcing), forcing, forcing, whole(forcing * forcing))
    return lax.fori_loop(0, ITERS, step, state)[:2]


def body(n_lat, n_lon, innovation, error, offset, cell, owner, count, land, inertia, depth):
    tiles = n_lat * n_lon
    rows, cols = 2 * land.shape[0], land.shape[1]
    vmem = pl.BlockSpec(memory_space=pltpu.VMEM)
    send = pl.pallas_call(
        functools.partial(arrange, tiles),
        out_shape=jax.ShapeDtypeStruct((tiles * ROWS, LANE), F32),
        in_specs=[vmem] * 5 + [pl.BlockSpec(memory_space=pltpu.SMEM)],
        out_specs=vmem,
    )(innovation, error, offset, cell, owner, count)
    recv = lax.all_to_all(
        send.reshape(tiles, ROWS, LANE), ("lat", "lon"), split_axis=0, concat_axis=0, tiled=True
    ).reshape(tiles * ROWS, LANE)
    part = pl.pallas_call(
        functools.partial(spread_kernel, rows, cols),
        out_shape=jax.ShapeDtypeStruct((2, rows // 2 + EDGE, cols + LANE), F32),
        in_specs=[vmem],
        out_specs=vmem,
        scratch_shapes=[pltpu.VMEM(total_shape(rows, cols), F32)],
    )(recv)
    field, residual, forcing, sound = solve(n_lat, n_lon, part, land, inertia, depth)
    return lax.cond(
        sound[0, 0] > 0.5,
        lambda: (field, residual),
        lambda: stepwise(forcing, land, inertia, depth),
    )


def solution(mesh):
    split = ("lat", "lon", "obs")
    grid = P(("lat", "obs"), "lon")
    return jax.shard_map(
        functools.partial(body, mesh.shape["lat"], mesh.shape["lon"]),
        mesh=mesh,
        in_specs=(
            P(split, None),
            P(split, None),
            P(None, split, None),
            P(split, None),
            P(split, None),
            P(split),
            grid,
            grid,
            grid,
        ),
        out_specs=(grid, grid),
        check_vma=False,
    )
```

```python
import functools

import jax
import jax.numpy as jnp
from jax import lax
from jax.experimental import pallas as pl
from jax.experimental.pallas import tpu as pltpu
from jax.sharding import PartitionSpec as P

ITERS = 5
CAP = 3
FIELDS = 4
ROWS = CAP * FIELDS
GROUP = 4
SPLIT = 4
PART = SPLIT + 1
LANE = 128
EDGE = 8
F32 = jnp.float32
BF16 = jnp.bfloat16
MESH = pl.DeviceIdType.MESH
CENTRE = 9.0
RADIUS = 9.0
TRUST = 1000.0


def iota(shape, dim):
    return lax.broadcasted_iota(jnp.int32, shape, dim)


def arrange(tiles, innovation, error, offset, cell, owner, count, send):
    blocks = innovation.shape[0]
    slots = tiles * CAP
    owners = owner[...]
    live = count[0]
    row, col = iota((blocks, blocks), 0), iota((blocks, blocks), 1)
    owners_f = owners.astype(F32)
    owners_col = jnp.sum(jnp.where(row == col, owners_f, 0.0), axis=1, keepdims=True)
    earlier = (owners_col == owners_f) & (row < col) & (row < live)
    rank = jnp.sum(jnp.where(earlier, 1.0, 0.0), axis=0, keepdims=True)
    lane = iota((1, blocks), 1)
    target = jnp.where(lane < live, owners_f * CAP + rank, -1.0)
    pick = jnp.where(iota((slots, blocks), 0).astype(F32) == target, 1.0, 0.0).astype(BF16)
    err = error[...]
    rest = jnp.concatenate(
        [innovation[...] / (err * err), offset[0], offset[1], cell[...].astype(F32)], axis=1
    )
    out = None
    for _ in range(3):
        part = rest.astype(BF16)
        term = jnp.dot(pick, part, preferred_element_type=F32)
        out = term if out is None else out + term
        rest = rest - part.astype(F32)
    for f in range(FIELDS):
        send[pl.ds(f, slots, stride=FIELDS), :] = out[:, f * LANE : (f + 1) * LANE]


def weigh(values, at, rows, cols, lhs, rhs):
    amount, north, east = values[0:1], values[1:2], values[2:3]
    cell = values[3:4].astype(jnp.int32)
    cell_row = cell // cols
    cell_col = cell % cols
    part = cell_col % SPLIT
    spot = iota((8, LANE), 0)
    across = jnp.where(spot == part, 1.0 - east, jnp.where(spot == part + 1, east, 0.0)) * amount
    down_at = iota((rows, LANE), 0)
    down = jnp.where(down_at == cell_row, 1.0 - north, jnp.where(down_at == cell_row + 1, north, 0.0))
    below = jnp.where(cell_row == rows - 1, north, 0.0) * across
    pieces = [down * across[c : c + 1] for c in range(PART)]
    pieces.append(jnp.concatenate([below, jnp.zeros((8, LANE), F32)], axis=0))
    second = PART * rows + 16
    lanes = slice(at, at + LANE)
    for c, piece in enumerate(pieces):
        high = piece.astype(BF16)
        low = (piece - high.astype(F32)).astype(BF16)
        end = c * rows + piece.shape[0]
        lhs[c * rows : end, lanes] = high
        lhs[second + c * rows : second + end, lanes] = low
    hot = jnp.where(iota((cols // SPLIT, LANE), 0) == cell_col // SPLIT, 1.0, 0.0)
    rhs[:, lanes] = hot.astype(BF16)


def weigh_group(recv, start, rows, cols, lhs, rhs):
    for i in range(0, GROUP * ROWS, 8):
        pair = recv[pl.ds(pl.multiple_of(start + i, 8), 8), :]
        for k in range(0, 8, FIELDS):
            weigh(pair[k : k + FIELDS], (i + k) // FIELDS * LANE, rows, cols, lhs, rhs)


def add_group(lhs, rhs, total):
    total[...] += lax.dot_general(
        lhs[...], rhs[...], (((1,), (1,)), ((), ())), preferred_element_type=F32
    )


def total_shape(rows, cols):
    return (2 * (PART * rows + 16), cols // SPLIT)


def unpack(total, rows, cols, part):
    wide = cols // SPLIT
    half = rows // 2
    count = PART * rows + 16
    acc = total[0:count, :] + total[count : 2 * count, :]
    under = acc[PART * rows : PART * rows + 8]
    top = iota((8, wide), 0) == 0
    fields = []
    for c in range(PART):
        row = jnp.where(top, jnp.broadcast_to(under[c : c + 1], (8, wide)), 0.0)
        fields.append(jnp.concatenate([acc[c * rows : (c + 1) * rows], row], axis=0))
    carried = pltpu.roll(fields[SPLIT], 1, 1)
    first = iota(carried.shape, 1) == 0
    past = jnp.where(first, carried, 0.0)[:, :LANE]
    fields[0] = fields[0] + jnp.where(first, 0.0, carried)
    size = SPLIT * LANE
    source, place = iota((size, size), 0), iota((size, size), 1)
    order = jnp.where(place == SPLIT * (source % LANE) + source // LANE, 1.0, 0.0).astype(BF16)
    strips = []
    for j in range(wide // LANE):
        rest = jnp.concatenate([f[:, j * LANE : (j + 1) * LANE] for f in fields[:SPLIT]], axis=1)
        out = None
        for _ in range(3):
            piece = rest.astype(BF16)
            term = jnp.dot(piece, order, preferred_element_type=F32)
            out = term if out is None else out + term
            rest = rest - piece.astype(F32)
        strips.append(out)
    for j, out in enumerate(strips):
        at = slice(j * size, (j + 1) * size)
        part[0, 0:half, at] = out[0:half]
        part[0, half : half + 8, at] = jnp.zeros((8, size), F32)
        part[1, :, at] = out[half:]
    part[0, 0:half, cols:] = past[0:half]
    part[0, half : half + 8, cols:] = jnp.zeros((8, LANE), F32)
    part[1, :, cols:] = past[half:]


def add_up(values):
    while len(values) > 1:
        rest = values[len(values) & ~1 :]
        values = [values[i] + values[i + 1] for i in range(0, len(values) - 1, 2)] + rest
    return values[0]


def coefficients(mu):
    start = mu[0]
    mu = [m / start for m in mu]
    gram = {}
    for s in range(2 * ITERS + 1):
        for d in range(s + 1):
            gram[s, d] = 0.5 * (mu[s] + mu[d])

    def inner(a, b):
        terms = [a[i] * b[j] * gram[i + j, abs(i - j)] for i in range(len(a)) for j in range(len(b))]
        return add_up(terms)

    def operate(a):
        out = [CENTRE * v for v in a] + [None]
        for i, v in enumerate(a):
            for j, f in ((1, RADIUS),) if i == 0 else ((i + 1, RADIUS / 2), (i - 1, RADIUS / 2)):
                out[j] = f * v if out[j] is None else out[j] + f * v
        return out

    one = jnp.ones_like(start)
    field, residual, direction = [], [one], [one]
    norm = one
    worst = one
    for _ in range(ITERS):
        applied = operate(direction)
        step = norm / inner(direction, applied)
        field = [
            step * d + (field[i] if i < len(field) else 0.0) for i, d in enumerate(direction)
        ]
        residual = [
            (residual[i] if i < len(residual) else 0.0) - step * a for i, a in enumerate(applied)
        ]
        after = inner(residual, residual)
        size = add_up([jnp.abs(v) for v in residual])
        worst = jnp.maximum(worst, jnp.where(after > 0, size * size / after, 1e30))
        ratio = after / norm
        direction = [
            v + (ratio * direction[i] if i < len(direction) else 0.0) for i, v in enumerate(residual)
        ]
        norm = after
    sound = jnp.where(worst < TRUST, 1.0, 0.0)
    return field, residual, sound


def step_kernel(
    n_lat,
    n_lon,
    innovation,
    error,
    offset,
    cell,
    owner,
    count,
    land,
    inertia,
    depth,
    field_out,
    residual_out,
    forcing_out,
    sound_out,
    send,
    recv,
    lhs_a,
    rhs_a,
    lhs_b,
    rhs_b,
    total,
    part,
    got,
    mine,
    west,
    east,
    tall,
    above,
    below,
    coef,
    cond,
    basis,
    line_in,
    line_at,
    rank_in,
    rank_at,
    out_sem,
    in_sem,
    send_sem,
    recv_sem,
    line_send,
    line_recv,
    rank_send,
    rank_recv,
):
    rows, cols = land.shape
    high, wide = rows + 2 * EDGE, cols + 2 * LANE
    lat, lon, obs = lax.axis_index("lat"), lax.axis_index("lon"), lax.axis_index("obs")
    tiles = n_lat * n_lon
    ranks = 2 * n_lat
    rank = lat * 2 + obs
    quads = n_lon // GROUP
    groups = n_lat * quads

    def on_line(k):
        return {"lon": k}

    def on_rank(k):
        return {"lat": k // 2, "obs": k % 2}

    def on_tile(k):
        return {"lat": k // n_lon, "lon": k % n_lon}

    me = lat * n_lon + lon
    barrier = pltpu.get_barrier_semaphore()

    def greet_tile(d, carry):
        pl.semaphore_signal(barrier, 1, device_id=on_tile((me + d) % tiles), device_id_type=MESH)
        return carry

    def greet_other(d, carry):
        device = {"lat": (lat + d) % n_lat, "obs": 1 - obs}
        pl.semaphore_signal(barrier, 1, device_id=device, device_id_type=MESH)
        return carry

    lax.fori_loop(1, tiles, greet_tile, 0)
    lax.fori_loop(0, n_lat, greet_other, 0)

    inner_rows, inner_cols = slice(EDGE, EDGE + rows), slice(LANE, LANE + cols)
    coef[0, inner_rows, inner_cols] = land[...].astype(F32) * depth[...]
    coef[1, inner_rows, inner_cols] = inertia[...]
    arrange(tiles, innovation, error, offset, cell, owner, count, send)
    pl.semaphore_wait(barrier, tiles - 1 + n_lat)

    def copy(k, src, dst, device):
        c = pltpu.make_async_remote_copy(
            src_ref=src,
            dst_ref=dst,
            send_sem=send_sem.at[k],
            recv_sem=recv_sem.at[k],
            device_id=device,
            device_id_type=MESH,
        )
        c.start()
        return c

    to_east, to_west = on_line((lon + 1) % n_lon), on_line((lon + n_lon - 1) % n_lon)
    to_south, to_north = on_rank((rank + 1) % ranks), on_rank((rank + ranks - 1) % ranks)
    own = pl.ds(EDGE, rows)

    coef_e = copy(1, coef.at[:, own, pl.ds(cols, LANE)], coef.at[:, own, pl.ds(0, LANE)], to_east)
    coef_w = copy(2, coef.at[:, own, pl.ds(LANE, LANE)], coef.at[:, own, pl.ds(LANE + cols, LANE)], to_west)

    def away(t):
        j = t // quads
        return (j % 2) * ((j + 1) // 2) + (1 - j % 2) * (n_lat - j // 2)

    def rows_of(k):
        return pl.ds(k * ROWS, ROWS)

    my_group = lat * quads + lon // GROUP

    def deliver(n, carry):
        t, d = n // GROUP, n % GROUP
        to_lat = (lat + n_lat - away(t) % n_lat) % n_lat
        to_quad = (lon // GROUP + quads - t % quads) % quads
        target = to_lat * n_lon + to_quad * GROUP + (lon + d) % GROUP
        pltpu.make_async_remote_copy(
            src_ref=send.at[rows_of(target), :],
            dst_ref=recv.at[rows_of(me), :],
            send_sem=out_sem,
            recv_sem=in_sem.at[my_group],
            device_id=on_tile(target),
            device_id_type=MESH,
        ).start()
        return carry

    pltpu.make_async_copy(send.at[rows_of(me), :], recv.at[rows_of(me), :], in_sem.at[my_group]).start()
    lax.fori_loop(1, tiles, deliver, 0)
    total[...] = jnp.zeros_like(total)
    height = GROUP * ROWS

    def group_of(t):
        from_lat = (lat + away(t)) % n_lat
        from_quad = (lon // GROUP + t % quads) % quads
        return from_lat * quads + from_quad

    def await_group(t):
        g = group_of(t)
        landed = recv.at[pl.ds(pl.multiple_of(g * height, 8), height), :]
        pltpu.make_async_copy(landed, landed, in_sem.at[g]).wait()

    def weigh_next(t, lhs, rhs):
        weigh_group(recv, group_of(t) * height, 2 * rows, cols, lhs, rhs)

    await_group(0)
    weigh_next(0, lhs_a, rhs_a)

    def spread_two(i, carry):
        await_group(2 * i + 1)
        weigh_next(2 * i + 1, lhs_b, rhs_b)
        add_group(lhs_a, rhs_a, total)
        following = jnp.minimum(2 * i + 2, groups - 1)

        @pl.when(i < groups // 2 - 1)
        def _():
            await_group(following)

        weigh_next(following, lhs_a, rhs_a)
        add_group(lhs_b, rhs_b, total)
        return carry

    lax.fori_loop(0, groups // 2, spread_two, 0)
    gone = send.at[pl.ds(0, (tiles - 1) * ROWS), :]
    pltpu.make_async_copy(gone, gone, out_sem).wait()
    unpack(total, 2 * rows, cols, part)

    coef_e.wait_recv()
    coef_w.wait_recv()
    coef_s = copy(5, coef.at[:, pl.ds(rows, EDGE), :], coef.at[:, pl.ds(0, EDGE), :], to_south)
    coef_n = copy(6, coef.at[:, pl.ds(EDGE, EDGE), :], coef.at[:, pl.ds(EDGE + rows, EDGE), :], to_north)
    pair = copy(0, part.at[1 - obs], got, {"obs": 1 - obs})
    pair.wait_recv()
    mine[...] = part[obs] + got[...]
    mine_e = copy(3, mine.at[:, pl.ds(cols - LANE, 2 * LANE)], west, to_east)
    mine_w = copy(4, mine.at[:, pl.ds(0, LANE)], east, to_west)
    mine_e.wait_recv()
    mine_w.wait_recv()
    tall[:, 0:LANE] = west[:, 0:LANE]
    tall[:, LANE : 2 * LANE] = mine[:, 0:LANE] + west[:, LANE:]
    tall[:, 2 * LANE : LANE + cols] = mine[:, LANE:cols]
    tall[:, LANE + cols :] = mine[:, cols:] + east[...]
    tall_s = copy(7, tall.at[pl.ds(rows - EDGE, 2 * EDGE), :], above, to_south)
    tall_n = copy(8, tall.at[pl.ds(0, EDGE), :], below, to_north)
    coef_s.wait_recv()
    coef_n.wait_recv()
    conduct = coef[0]
    north = jnp.sqrt(conduct * pltpu.roll(conduct, 1, 0))
    south = pltpu.roll(north, high - 1, 0)
    left = jnp.sqrt(conduct * pltpu.roll(conduct, 1, 1))
    right = pltpu.roll(left, wide - 1, 1)
    cond[0] = (coef[1] + north + south + left + right - CENTRE) * (1.0 / RADIUS)
    cond[1] = north * (1.0 / RADIUS)
    cond[2] = south * (1.0 / RADIUS)
    cond[3] = left * (1.0 / RADIUS)
    cond[4] = right * (1.0 / RADIUS)
    tall_s.wait_recv()
    tall_n.wait_recv()
    ocean = coef[0] > 0
    raw = jnp.concatenate(
        [
            above[0:EDGE, :],
            tall[0:EDGE, :] + above[EDGE:, :],
            tall[EDGE:rows, :],
            below[...] + tall[rows:, :],
        ],
        axis=0,
    )
    basis[0] = jnp.where(ocean, raw, 0.0)
    forcing_out[...] = basis[0, inner_rows, inner_cols]

    def operate(v):
        return (
            cond[0] * v
            - cond[1] * pltpu.roll(v, 1, 0)
            - cond[2] * pltpu.roll(v, high - 1, 0)
            - cond[3] * pltpu.roll(v, 1, 1)
            - cond[4] * pltpu.roll(v, wide - 1, 1)
        )

    for k in range(ITERS):
        after = operate(basis[k])
        basis[k + 1] = after if k == 0 else 2.0 * after - basis[k - 1]

    def dot(i, j):
        pieces = []
        for a in range(EDGE, EDGE + rows, 8):
            for b in range(LANE, LANE + cols, LANE):
                pieces.append(basis[i, a : a + 8, b : b + LANE] * basis[j, a : a + 8, b : b + LANE])
        return jnp.sum(add_up(pieces), axis=0, keepdims=True)

    pairs = [(k // 2, (k + 1) // 2) for k in range(2 * ITERS + 1)]
    sums = [dot(i, j) for i, j in pairs]
    stack = jnp.concatenate(sums + [jnp.zeros((16 - len(sums), LANE), F32)], axis=0)
    column = jnp.sum(stack, axis=1, keepdims=True)
    diag = iota((16, LANE), 0) == iota((16, LANE), 1)
    line_in[...] = jnp.sum(jnp.where(diag, column, 0.0), axis=0, keepdims=True)

    def share(count, me, device, value, at, s_sem, r_sem):
        def copy_of(slot, k, target):
            return pltpu.make_async_remote_copy(
                src_ref=value,
                dst_ref=at.at[slot],
                send_sem=s_sem.at[k],
                recv_sem=r_sem.at[slot],
                device_id=device(target),
                device_id_type=MESH,
            )

        def begin(d, carry):
            copy_of(me, d, (me + d) % count).start()
            return carry

        def arrive(d, carry):
            copy_of((me + count - d) % count, d, (me + d) % count).wait_recv()
            return carry

        def leave(d, carry):
            copy_of(me, d, (me + d) % count).wait_send()
            return carry

        lax.fori_loop(1, count, begin, 0)
        at[me] = value[...]
        lax.fori_loop(1, count, arrive, 0)
        lax.fori_loop(1, count, leave, 0)
        return add_up([at[k] for k in range(count)])

    rank_in[...] = share(n_lon, lon, on_line, line_in, line_at, line_send, line_recv)
    sums = share(ranks, rank, on_rank, rank_in, rank_at, rank_send, rank_recv)
    lane = iota((1, LANE), 1)
    raw_sums = [
        jnp.sum(jnp.where(lane == k, sums, 0.0), axis=1, keepdims=True) for k in range(2 * ITERS + 1)
    ]
    mu = [
        raw_sums[k] if k < 2 else 2.0 * raw_sums[k] - raw_sums[k % 2] for k in range(2 * ITERS + 1)
    ]
    field, residual, sound = coefficients(mu)
    views = [basis[k, inner_rows, inner_cols] for k in range(ITERS + 1)]
    field_out[...] = add_up([c * v for c, v in zip(field, views)])
    residual_out[...] = add_up([c * v for c, v in zip(residual, views)])
    sound_out[...] = jnp.broadcast_to(sound, (1, LANE))
    for c in (pair, coef_e, coef_w, mine_e, mine_w, coef_s, coef_n, tall_s, tall_n):
        c.wait_send()


def step(n_lat, n_lon, innovation, error, offset, cell, owner, count, land, inertia, depth):
    rows, cols = land.shape
    high, wide = rows + 2 * EDGE, cols + 2 * LANE
    own = jax.ShapeDtypeStruct((rows, cols), F32)
    vmem = pl.BlockSpec(memory_space=pltpu.VMEM)
    ranks = 2 * n_lat
    tiles = n_lat * n_lon
    groups = tiles // GROUP
    tall = total_shape(2 * rows, cols)
    deep = GROUP * CAP * LANE
    return pl.pallas_call(
        functools.partial(step_kernel, n_lat, n_lon),
        out_shape=(own, own, own, jax.ShapeDtypeStruct((1, LANE), F32)),
        in_specs=[vmem] * 5 + [pl.BlockSpec(memory_space=pltpu.SMEM)] + [vmem] * 3,
        out_specs=(vmem,) * 4,
        scratch_shapes=[
            pltpu.VMEM((tiles * ROWS, LANE), F32),
            pltpu.VMEM((tiles * ROWS, LANE), F32),
            pltpu.VMEM((tall[0], deep), BF16),
            pltpu.VMEM((tall[1], deep), BF16),
            pltpu.VMEM((tall[0], deep), BF16),
            pltpu.VMEM((tall[1], deep), BF16),
            pltpu.VMEM(tall, F32),
            pltpu.VMEM((2, rows + EDGE, cols + LANE), F32),
            pltpu.VMEM((rows + EDGE, cols + LANE), F32),
            pltpu.VMEM((rows + EDGE, cols + LANE), F32),
            pltpu.VMEM((rows + EDGE, 2 * LANE), F32),
            pltpu.VMEM((rows + EDGE, LANE), F32),
            pltpu.VMEM((rows + EDGE, wide), F32),
            pltpu.VMEM((2 * EDGE, wide), F32),
            pltpu.VMEM((EDGE, wide), F32),
            pltpu.VMEM((2, high, wide), F32),
            pltpu.VMEM((5, high, wide), F32),
            pltpu.VMEM((ITERS + 1, high, wide), F32),
            pltpu.VMEM((1, LANE), F32),
            pltpu.VMEM((n_lon, 1, LANE), F32),
            pltpu.VMEM((1, LANE), F32),
            pltpu.VMEM((ranks, 1, LANE), F32),
            pltpu.SemaphoreType.DMA,
            pltpu.SemaphoreType.DMA((groups,)),
            pltpu.SemaphoreType.DMA((9,)),
            pltpu.SemaphoreType.DMA((9,)),
            pltpu.SemaphoreType.DMA((n_lon,)),
            pltpu.SemaphoreType.DMA((n_lon,)),
            pltpu.SemaphoreType.DMA((ranks,)),
            pltpu.SemaphoreType.DMA((ranks,)),
        ],
        compiler_params=pltpu.CompilerParams(collective_id=1, has_side_effects=True),
    )(innovation, error, offset, cell, owner, count, land, inertia, depth)


def shifted(value, axis, steps):
    count = lax.axis_size(axis)
    return lax.ppermute(value, axis, [(i, (i + steps) % count) for i in range(count)])


def border(block):
    for axis, dim in ((("lat", "obs"), 0), ("lon", 1)):
        size = block.shape[dim]
        low = shifted(lax.slice_in_dim(block, size - 1, size, axis=dim), axis, 1)
        high = shifted(lax.slice_in_dim(block, 0, 1, axis=dim), axis, -1)
        block = jnp.concatenate([low, block, high], axis=dim)
    return block


def stepwise(forcing, land, inertia, depth):
    conduct = land.astype(F32) * depth
    padded = border(conduct)
    north = jnp.sqrt(conduct * padded[:-2, 1:-1])
    south = jnp.sqrt(conduct * padded[2:, 1:-1])
    west = jnp.sqrt(conduct * padded[1:-1, :-2])
    east = jnp.sqrt(conduct * padded[1:-1, 2:])
    diagonal = inertia + north + south + west + east

    def whole(value):
        return lax.psum(jnp.sum(value), ("lat", "lon", "obs"))

    def step(_, state):
        field, residual, direction, norm = state
        outer = border(direction)
        applied = (
            diagonal * direction
            - north * outer[:-2, 1:-1]
            - south * outer[2:, 1:-1]
            - west * outer[1:-1, :-2]
            - east * outer[1:-1, 2:]
        )
        size = norm / whole(direction * applied)
        field = field + size * direction
        residual = residual - size * applied
        after = whole(residual * residual)
        return field, residual, residual + after / norm * direction, after

    state = (jnp.zeros_like(forcing), forcing, forcing, whole(forcing * forcing))
    return lax.fori_loop(0, ITERS, step, state)[:2]


def body(n_lat, n_lon, *inputs):
    land, inertia, depth = inputs[-3:]
    field, residual, forcing, sound = step(n_lat, n_lon, *inputs)
    return lax.cond(
        sound[0, 0] > 0.5,
        lambda: (field, residual),
        lambda: stepwise(forcing, land, inertia, depth),
    )


def solution(mesh):
    split = ("lat", "lon", "obs")
    grid = P(("lat", "obs"), "lon")
    return jax.shard_map(
        functools.partial(body, mesh.shape["lat"], mesh.shape["lon"]),
        mesh=mesh,
        in_specs=(
            P(split, None),
            P(split, None),
            P(None, split, None),
            P(split, None),
            P(split, None),
            P(split),
            grid,
            grid,
            grid,
        ),
        out_specs=(grid, grid),
        check_vma=False,
    )
```

```python
import functools

import jax
import jax.numpy as jnp
from jax import lax
from jax.experimental import pallas as pl
from jax.experimental.pallas import tpu as pltpu
from jax.sharding import PartitionSpec as P

ITERS = 5
CAP = 3
FIELDS = 4
ROWS = CAP * FIELDS
GROUP = 8
SPLIT = 4
PART = SPLIT + 1
LANE = 128
EDGE = 8
F32 = jnp.float32
BF16 = jnp.bfloat16
MESH = pl.DeviceIdType.MESH
CENTRE = 9.0
RADIUS = 9.0
TRUST = 1000.0


def iota(shape, dim):
    return lax.broadcasted_iota(jnp.int32, shape, dim)


def arrange(tiles, innovation, error, offset, cell, owner, count, send):
    blocks = innovation.shape[0]
    slots = tiles * CAP
    owners = owner[...]
    live = count[0]
    row, col = iota((blocks, blocks), 0), iota((blocks, blocks), 1)
    owners_f = owners.astype(F32)
    owners_col = jnp.sum(jnp.where(row == col, owners_f, 0.0), axis=1, keepdims=True)
    earlier = (owners_col == owners_f) & (row < col) & (row < live)
    rank = jnp.sum(jnp.where(earlier, 1.0, 0.0), axis=0, keepdims=True)
    lane = iota((1, blocks), 1)
    target = jnp.where(lane < live, owners_f * CAP + rank, -1.0)
    pick = jnp.where(iota((slots, blocks), 0).astype(F32) == target, 1.0, 0.0).astype(BF16)
    err = error[...]
    rest = jnp.concatenate(
        [innovation[...] / (err * err), offset[0], offset[1], cell[...].astype(F32)], axis=1
    )
    out = None
    for _ in range(3):
        part = rest.astype(BF16)
        term = jnp.dot(pick, part, preferred_element_type=F32)
        out = term if out is None else out + term
        rest = rest - part.astype(F32)
    for f in range(FIELDS):
        send[pl.ds(f, slots, stride=FIELDS), :] = out[:, f * LANE : (f + 1) * LANE]


def weigh(values, k, rows, cols, index, lhs, rhs):
    amount, north, east = values[0:1], values[1:2], values[2:3]
    cell = values[3:4].astype(jnp.int32)
    cell_row = lax.div(cell, cols)
    cell_col = lax.rem(cell, cols)
    part = lax.rem(cell_col, SPLIT)
    spot = iota((8, LANE), 0)
    across = jnp.where(spot == part, 1.0 - east, jnp.where(spot == part + 1, east, 0.0)) * amount
    down_at = iota((rows, LANE), 0)
    down = jnp.where(down_at == cell_row, 1.0 - north, jnp.where(down_at == cell_row + 1, north, 0.0))
    below = jnp.where(cell_row == rows - 1, north, 0.0) * across
    pieces = [down * across[c : c + 1] for c in range(PART)]
    pieces.append(jnp.concatenate([below, jnp.zeros((8, LANE), F32)], axis=0))
    second = PART * rows + 16
    for c, piece in enumerate(pieces):
        end = c * rows + piece.shape[0]
        main = piece.astype(BF16)
        lhs[k, c * rows : end, :] = main
        lhs[k, second + c * rows : second + end, :] = (piece - main.astype(F32)).astype(BF16)
    spots = index[...]
    column = lax.div(cell_col, SPLIT).astype(F32).astype(BF16)
    rhs[k] = jnp.where(spots == column, jnp.ones_like(spots), jnp.zeros_like(spots))


def weigh_group(recv, start, rows, cols, index, lhs, rhs):
    for i in range(0, GROUP * ROWS, 8):
        pair = recv[pl.ds(pl.multiple_of(start + i, 8), 8), :]
        for k in range(0, 8, FIELDS):
            weigh(pair[k : k + FIELDS], (i + k) // FIELDS, rows, cols, index, lhs, rhs)


def add_group(lhs, rhs, total):
    total[...] += lax.dot_general(
        jnp.concatenate([lhs[k] for k in range(lhs.shape[0])], axis=1),
        jnp.concatenate([rhs[k] for k in range(rhs.shape[0])], axis=1),
        (((1,), (1,)), ((), ())),
        preferred_element_type=F32,
    )


def total_shape(rows, cols):
    return (2 * (PART * rows + 16), cols // SPLIT)


def unpack(total, rows, cols, part):
    wide = cols // SPLIT
    half = rows // 2
    count = PART * rows + 16
    acc = total[0:count, :] + total[count : 2 * count, :]
    under = acc[PART * rows : PART * rows + 8]
    top = iota((8, wide), 0) == 0
    fields = []
    for c in range(PART):
        row = jnp.where(top, jnp.broadcast_to(under[c : c + 1], (8, wide)), 0.0)
        fields.append(jnp.concatenate([acc[c * rows : (c + 1) * rows], row], axis=0))
    carried = pltpu.roll(fields[SPLIT], 1, 1)
    first = iota(carried.shape, 1) == 0
    past = jnp.where(first, carried, 0.0)[:, :LANE]
    fields[0] = fields[0] + jnp.where(first, 0.0, carried)
    size = SPLIT * LANE
    source, place = iota((size, size), 0), iota((size, size), 1)
    order = jnp.where(place == SPLIT * (source % LANE) + source // LANE, 1.0, 0.0).astype(BF16)
    strips = []
    for j in range(wide // LANE):
        rest = jnp.concatenate([f[:, j * LANE : (j + 1) * LANE] for f in fields[:SPLIT]], axis=1)
        out = None
        for _ in range(3):
            piece = rest.astype(BF16)
            term = jnp.dot(piece, order, preferred_element_type=F32)
            out = term if out is None else out + term
            rest = rest - piece.astype(F32)
        strips.append(out)
    for j, out in enumerate(strips):
        at = slice(j * size, (j + 1) * size)
        part[0, 0:half, at] = out[0:half]
        part[0, half : half + 8, at] = jnp.zeros((8, size), F32)
        part[1, :, at] = out[half:]
    part[0, 0:half, cols:] = past[0:half]
    part[0, half : half + 8, cols:] = jnp.zeros((8, LANE), F32)
    part[1, :, cols:] = past[half:]


def add_up(values):
    while len(values) > 1:
        rest = values[len(values) & ~1 :]
        values = [values[i] + values[i + 1] for i in range(0, len(values) - 1, 2)] + rest
    return values[0]


def coefficients(mu):
    start = mu[0]
    mu = [m / start for m in mu]
    gram = {}
    for s in range(2 * ITERS + 1):
        for d in range(s + 1):
            gram[s, d] = 0.5 * (mu[s] + mu[d])

    def inner(a, b):
        terms = [a[i] * b[j] * gram[i + j, abs(i - j)] for i in range(len(a)) for j in range(len(b))]
        return add_up(terms)

    def operate(a):
        out = [CENTRE * v for v in a] + [None]
        for i, v in enumerate(a):
            for j, f in ((1, RADIUS),) if i == 0 else ((i + 1, RADIUS / 2), (i - 1, RADIUS / 2)):
                out[j] = f * v if out[j] is None else out[j] + f * v
        return out

    one = jnp.ones_like(start)
    field, residual, direction = [], [one], [one]
    norm = one
    worst = one
    for _ in range(ITERS):
        applied = operate(direction)
        step = norm / inner(direction, applied)
        field = [
            step * d + (field[i] if i < len(field) else 0.0) for i, d in enumerate(direction)
        ]
        residual = [
            (residual[i] if i < len(residual) else 0.0) - step * a for i, a in enumerate(applied)
        ]
        after = inner(residual, residual)
        size = add_up([jnp.abs(v) for v in residual])
        worst = jnp.maximum(worst, jnp.where(after > 0, size * size / after, 1e30))
        ratio = after / norm
        direction = [
            v + (ratio * direction[i] if i < len(direction) else 0.0) for i, v in enumerate(residual)
        ]
        norm = after
    sound = jnp.where(worst < TRUST, 1.0, 0.0)
    return field, residual, sound


def step_kernel(
    n_lat,
    n_lon,
    innovation,
    error,
    offset,
    cell,
    owner,
    count,
    land,
    inertia,
    depth,
    field_out,
    residual_out,
    forcing_out,
    sound_out,
    send,
    recv,
    lhs_a,
    rhs_a,
    lhs_b,
    rhs_b,
    index,
    total,
    part,
    got,
    mine,
    west,
    east,
    tall,
    above,
    below,
    coef,
    cond,
    basis,
    line_in,
    line_at,
    rank_in,
    rank_at,
    out_sem,
    in_sem,
    send_sem,
    recv_sem,
    line_send,
    line_recv,
    rank_send,
    rank_recv,
):
    rows, cols = land.shape
    high, wide = rows + 2 * EDGE, cols + 2 * LANE
    lat, lon, obs = lax.axis_index("lat"), lax.axis_index("lon"), lax.axis_index("obs")
    tiles = n_lat * n_lon
    ranks = 2 * n_lat
    rank = lat * 2 + obs
    quads = n_lon // GROUP
    groups = n_lat * quads

    def on_line(k):
        return {"lon": k}

    def on_rank(k):
        return {"lat": lax.div(k, 2), "obs": lax.rem(k, 2)}

    def on_tile(k):
        return {"lat": lax.div(k, n_lon), "lon": lax.rem(k, n_lon)}

    me = lat * n_lon + lon
    barrier = pltpu.get_barrier_semaphore()

    def greet_tile(d, carry):
        device = on_tile(lax.rem(me + d, tiles))
        pl.semaphore_signal(barrier, 1, device_id=device, device_id_type=MESH)
        return carry

    def greet_other(d, carry):
        device = {"lat": lax.rem(lat + d, n_lat), "obs": 1 - obs}
        pl.semaphore_signal(barrier, 1, device_id=device, device_id_type=MESH)
        return carry

    lax.fori_loop(1, tiles, greet_tile, 0)
    lax.fori_loop(0, n_lat, greet_other, 0)

    inner_rows, inner_cols = slice(EDGE, EDGE + rows), slice(LANE, LANE + cols)
    coef[0, inner_rows, inner_cols] = land[...].astype(F32) * depth[...]
    coef[1, inner_rows, inner_cols] = inertia[...]
    arrange(tiles, innovation, error, offset, cell, owner, count, send)
    pl.semaphore_wait(barrier, tiles - 1 + n_lat)

    def copy(k, src, dst, device):
        c = pltpu.make_async_remote_copy(
            src_ref=src,
            dst_ref=dst,
            send_sem=send_sem.at[k],
            recv_sem=recv_sem.at[k],
            device_id=device,
            device_id_type=MESH,
        )
        c.start()
        return c

    to_east, to_west = on_line(lax.rem(lon + 1, n_lon)), on_line(lax.rem(lon + n_lon - 1, n_lon))
    to_south, to_north = on_rank(lax.rem(rank + 1, ranks)), on_rank(lax.rem(rank + ranks - 1, ranks))
    own = pl.ds(EDGE, rows)

    coef_e = copy(1, coef.at[:, own, pl.ds(cols, LANE)], coef.at[:, own, pl.ds(0, LANE)], to_east)
    coef_w = copy(2, coef.at[:, own, pl.ds(LANE, LANE)], coef.at[:, own, pl.ds(LANE + cols, LANE)], to_west)

    quad, place = lax.div(lon, GROUP), lax.rem(lon, GROUP)

    def away(t):
        j = lax.div(t, quads)
        odd = lax.rem(j, 2)
        return lax.rem(odd * lax.div(j + 1, 2) + (1 - odd) * (n_lat - lax.div(j, 2)), n_lat)

    def rows_of(k):
        return pl.ds(k * ROWS, ROWS)

    my_group = lat * quads + quad

    def deliver(t, carry):
        to_lat = lax.rem(lat + n_lat - away(t), n_lat)
        to_quad = lax.rem(quad + quads - lax.rem(t, quads), quads)
        for d in range(GROUP):
            to_lon = to_quad * GROUP + lax.rem(place + d, GROUP)
            transfer = pltpu.make_async_remote_copy(
                src_ref=send.at[rows_of(to_lat * n_lon + to_lon), :],
                dst_ref=recv.at[rows_of(me), :],
                send_sem=out_sem,
                recv_sem=in_sem.at[my_group],
                device_id={"lat": to_lat, "lon": to_lon},
                device_id_type=MESH,
            )
            if d:
                transfer.start()
            else:
                pl.when(t > 0)(transfer.start)
        return carry

    pltpu.make_async_copy(send.at[rows_of(me), :], recv.at[rows_of(me), :], in_sem.at[my_group]).start()
    lax.fori_loop(0, groups, deliver, 0)
    total[...] = jnp.zeros_like(total)
    index[...] = iota(index.shape, 0).astype(F32).astype(BF16)
    height = GROUP * ROWS

    def group_of(t):
        from_lat = lax.rem(lat + away(t), n_lat)
        return from_lat * quads + lax.rem(quad + lax.rem(t, quads), quads)

    def await_group(t):
        g = group_of(t)
        landed = recv.at[pl.ds(pl.multiple_of(g * height, 8), height), :]
        pltpu.make_async_copy(landed, landed, in_sem.at[g]).wait()

    def weigh_next(t, lhs, rhs):
        weigh_group(recv, group_of(t) * height, 2 * rows, cols, index, lhs, rhs)

    await_group(0)
    weigh_next(0, lhs_a, rhs_a)

    def spread_two(i, carry):
        await_group(2 * i + 1)
        weigh_next(2 * i + 1, lhs_b, rhs_b)
        add_group(lhs_a, rhs_a, total)
        await_group(2 * i + 2)
        weigh_next(2 * i + 2, lhs_a, rhs_a)
        add_group(lhs_b, rhs_b, total)
        return carry

    lax.fori_loop(0, groups // 2 - 1, spread_two, 0)
    await_group(groups - 1)
    weigh_next(groups - 1, lhs_b, rhs_b)
    add_group(lhs_a, rhs_a, total)
    add_group(lhs_b, rhs_b, total)
    gone = send.at[pl.ds(0, (tiles - 1) * ROWS), :]
    pltpu.make_async_copy(gone, gone, out_sem).wait()
    unpack(total, 2 * rows, cols, part)

    coef_e.wait_recv()
    coef_w.wait_recv()
    coef_s = copy(5, coef.at[:, pl.ds(rows, EDGE), :], coef.at[:, pl.ds(0, EDGE), :], to_south)
    coef_n = copy(6, coef.at[:, pl.ds(EDGE, EDGE), :], coef.at[:, pl.ds(EDGE + rows, EDGE), :], to_north)
    pair = copy(0, part.at[1 - obs], got, {"obs": 1 - obs})
    pair.wait_recv()
    mine[...] = part[obs] + got[...]
    mine_e = copy(3, mine.at[:, pl.ds(cols - LANE, 2 * LANE)], west, to_east)
    mine_w = copy(4, mine.at[:, pl.ds(0, LANE)], east, to_west)
    mine_e.wait_recv()
    mine_w.wait_recv()
    tall[:, 0:LANE] = west[:, 0:LANE]
    tall[:, LANE : 2 * LANE] = mine[:, 0:LANE] + west[:, LANE:]
    tall[:, 2 * LANE : LANE + cols] = mine[:, LANE:cols]
    tall[:, LANE + cols :] = mine[:, cols:] + east[...]
    tall_s = copy(7, tall.at[pl.ds(rows - EDGE, 2 * EDGE), :], above, to_south)
    tall_n = copy(8, tall.at[pl.ds(0, EDGE), :], below, to_north)
    coef_s.wait_recv()
    coef_n.wait_recv()
    conduct = coef[0]
    north = jnp.sqrt(conduct * pltpu.roll(conduct, 1, 0))
    south = pltpu.roll(north, high - 1, 0)
    left = jnp.sqrt(conduct * pltpu.roll(conduct, 1, 1))
    right = pltpu.roll(left, wide - 1, 1)
    cond[0] = (coef[1] + north + south + left + right - CENTRE) * (1.0 / RADIUS)
    cond[1] = north * (1.0 / RADIUS)
    cond[2] = south * (1.0 / RADIUS)
    cond[3] = left * (1.0 / RADIUS)
    cond[4] = right * (1.0 / RADIUS)
    tall_s.wait_recv()
    tall_n.wait_recv()
    ocean = coef[0] > 0
    raw = jnp.concatenate(
        [
            above[0:EDGE, :],
            tall[0:EDGE, :] + above[EDGE:, :],
            tall[EDGE:rows, :],
            below[...] + tall[rows:, :],
        ],
        axis=0,
    )
    basis[0] = jnp.where(ocean, raw, 0.0)
    forcing_out[...] = basis[0, inner_rows, inner_cols]

    def operate(v):
        return (
            cond[0] * v
            - cond[1] * pltpu.roll(v, 1, 0)
            - cond[2] * pltpu.roll(v, high - 1, 0)
            - cond[3] * pltpu.roll(v, 1, 1)
            - cond[4] * pltpu.roll(v, wide - 1, 1)
        )

    for k in range(ITERS):
        after = operate(basis[k])
        basis[k + 1] = after if k == 0 else 2.0 * after - basis[k - 1]

    def dot(i, j):
        pieces = []
        for a in range(EDGE, EDGE + rows, 8):
            for b in range(LANE, LANE + cols, LANE):
                pieces.append(basis[i, a : a + 8, b : b + LANE] * basis[j, a : a + 8, b : b + LANE])
        return jnp.sum(add_up(pieces), axis=0, keepdims=True)

    pairs = [(k // 2, (k + 1) // 2) for k in range(2 * ITERS + 1)]
    sums = [dot(i, j) for i, j in pairs]
    stack = jnp.concatenate(sums + [jnp.zeros((16 - len(sums), LANE), F32)], axis=0)
    column = jnp.sum(stack, axis=1, keepdims=True)
    diag = iota((16, LANE), 0) == iota((16, LANE), 1)
    line_in[...] = jnp.sum(jnp.where(diag, column, 0.0), axis=0, keepdims=True)

    def share(count, me, device, value, at, s_sem, r_sem):
        def copy_of(slot, k, target):
            return pltpu.make_async_remote_copy(
                src_ref=value,
                dst_ref=at.at[slot],
                send_sem=s_sem.at[k],
                recv_sem=r_sem.at[slot],
                device_id=device(target),
                device_id_type=MESH,
            )

        half = count // 2
        offsets = [half] + [half + s * k for k in range(1, half) for s in (1, -1)]
        for d in offsets:
            copy_of(me, d, lax.rem(me + d, count)).start()
        at[me] = value[...]
        for d in reversed(offsets):
            copy_of(lax.rem(me + count - d, count), d, lax.rem(me + d, count)).wait_recv()
        for d in offsets:
            copy_of(me, d, lax.rem(me + d, count)).wait_send()
        return add_up([at[k] for k in range(count)])

    rank_in[...] = share(n_lon, lon, on_line, line_in, line_at, line_send, line_recv)
    sums = share(ranks, rank, on_rank, rank_in, rank_at, rank_send, rank_recv)
    lane = iota((1, LANE), 1)
    raw_sums = [
        jnp.sum(jnp.where(lane == k, sums, 0.0), axis=1, keepdims=True) for k in range(2 * ITERS + 1)
    ]
    mu = [
        raw_sums[k] if k < 2 else 2.0 * raw_sums[k] - raw_sums[k % 2] for k in range(2 * ITERS + 1)
    ]
    field, residual, sound = coefficients(mu)
    views = [basis[k, inner_rows, inner_cols] for k in range(ITERS + 1)]
    field_out[...] = add_up([c * v for c, v in zip(field, views)])
    residual_out[...] = add_up([c * v for c, v in zip(residual, views)])
    sound_out[...] = jnp.broadcast_to(sound, (1, LANE))
    for c in (pair, coef_e, coef_w, mine_e, mine_w, coef_s, coef_n, tall_s, tall_n):
        c.wait_send()


def step(n_lat, n_lon, innovation, error, offset, cell, owner, count, land, inertia, depth):
    rows, cols = land.shape
    high, wide = rows + 2 * EDGE, cols + 2 * LANE
    own = jax.ShapeDtypeStruct((rows, cols), F32)
    vmem = pl.BlockSpec(memory_space=pltpu.VMEM)
    ranks = 2 * n_lat
    tiles = n_lat * n_lon
    groups = tiles // GROUP
    tall = total_shape(2 * rows, cols)
    deep = GROUP * CAP
    return pl.pallas_call(
        functools.partial(step_kernel, n_lat, n_lon),
        out_shape=(own, own, own, jax.ShapeDtypeStruct((1, LANE), F32)),
        in_specs=[vmem] * 5 + [pl.BlockSpec(memory_space=pltpu.SMEM)] + [vmem] * 3,
        out_specs=(vmem,) * 4,
        scratch_shapes=[
            pltpu.VMEM((tiles * ROWS, LANE), F32),
            pltpu.VMEM((tiles * ROWS, LANE), F32),
            pltpu.VMEM((deep, tall[0], LANE), BF16),
            pltpu.VMEM((deep, tall[1], LANE), BF16),
            pltpu.VMEM((deep, tall[0], LANE), BF16),
            pltpu.VMEM((deep, tall[1], LANE), BF16),
            pltpu.VMEM((tall[1], LANE), BF16),
            pltpu.VMEM(tall, F32),
            pltpu.VMEM((2, rows + EDGE, cols + LANE), F32),
            pltpu.VMEM((rows + EDGE, cols + LANE), F32),
            pltpu.VMEM((rows + EDGE, cols + LANE), F32),
            pltpu.VMEM((rows + EDGE, 2 * LANE), F32),
            pltpu.VMEM((rows + EDGE, LANE), F32),
            pltpu.VMEM((rows + EDGE, wide), F32),
            pltpu.VMEM((2 * EDGE, wide), F32),
            pltpu.VMEM((EDGE, wide), F32),
            pltpu.VMEM((2, high, wide), F32),
            pltpu.VMEM((5, high, wide), F32),
            pltpu.VMEM((ITERS + 1, high, wide), F32),
            pltpu.VMEM((1, LANE), F32),
            pltpu.VMEM((n_lon, 1, LANE), F32),
            pltpu.VMEM((1, LANE), F32),
            pltpu.VMEM((ranks, 1, LANE), F32),
            pltpu.SemaphoreType.DMA,
            pltpu.SemaphoreType.DMA((groups,)),
            pltpu.SemaphoreType.DMA((9,)),
            pltpu.SemaphoreType.DMA((9,)),
            pltpu.SemaphoreType.DMA((n_lon,)),
            pltpu.SemaphoreType.DMA((n_lon,)),
            pltpu.SemaphoreType.DMA((ranks,)),
            pltpu.SemaphoreType.DMA((ranks,)),
        ],
        compiler_params=pltpu.CompilerParams(collective_id=1, has_side_effects=True),
    )(innovation, error, offset, cell, owner, count, land, inertia, depth)


def shifted(value, axis, steps):
    count = lax.axis_size(axis)
    return lax.ppermute(value, axis, [(i, (i + steps) % count) for i in range(count)])


def border(block):
    for axis, dim in ((("lat", "obs"), 0), ("lon", 1)):
        size = block.shape[dim]
        low = shifted(lax.slice_in_dim(block, size - 1, size, axis=dim), axis, 1)
        high = shifted(lax.slice_in_dim(block, 0, 1, axis=dim), axis, -1)
        block = jnp.concatenate([low, block, high], axis=dim)
    return block


def stepwise(sound, field, residual, forcing, land, own, sea):
    def whole(value):
        return lax.psum(jnp.sum(value), ("lat", "lon", "obs"))

    def step(_, state):
        (field, residual, direction, before), depth, inertia = lax.optimization_barrier(
            (state, sea, own)
        )
        conduct = land.astype(F32) * depth
        padded = border(conduct)
        north = jnp.sqrt(conduct * padded[:-2, 1:-1])
        south = jnp.sqrt(conduct * padded[2:, 1:-1])
        west = jnp.sqrt(conduct * padded[1:-1, :-2])
        east = jnp.sqrt(conduct * padded[1:-1, 2:])
        diagonal = inertia + north + south + west + east
        norm = whole(residual * residual)
        direction = residual + norm / before * direction
        outer = border(direction)
        applied = (
            diagonal * direction
            - north * outer[:-2, 1:-1]
            - south * outer[2:, 1:-1]
            - west * outer[1:-1, :-2]
            - east * outer[1:-1, 2:]
        )
        size = norm / whole(direction * applied)
        return field + size * direction, residual - size * applied, direction, norm

    state = (
        jnp.where(sound, field, 0.0),
        jnp.where(sound, residual, forcing),
        jnp.zeros_like(forcing),
        jnp.float32(1.0),
    )
    return lax.fori_loop(0, jnp.where(sound, 0, ITERS), step, state)[:2]


def body(n_lat, n_lon, *inputs):
    land, inertia, depth = inputs[-3:]
    field, residual, forcing, sound = step(n_lat, n_lon, *inputs)
    return stepwise(sound[0, 0] > 0.5, field, residual, forcing, land, inertia, depth)


def solution(mesh):
    split = ("lat", "lon", "obs")
    grid = P(("lat", "obs"), "lon")
    return jax.shard_map(
        functools.partial(body, mesh.shape["lat"], mesh.shape["lon"]),
        mesh=mesh,
        in_specs=(
            P(split, None),
            P(split, None),
            P(None, split, None),
            P(split, None),
            P(split, None),
            P(split),
            grid,
            grid,
            grid,
        ),
        out_specs=(grid, grid),
        check_vma=False,
    )
```

```python
import functools

import jax
import jax.numpy as jnp
from jax import lax
from jax.experimental import pallas as pl
from jax.experimental.pallas import tpu as pltpu
from jax.sharding import PartitionSpec as P

ITERS = 5
CAP = 3
FIELDS = 4
ROWS = CAP * FIELDS
GROUP = 8
SPLIT = 4
PART = SPLIT + 1
LANE = 128
EDGE = 8
F32 = jnp.float32
BF16 = jnp.bfloat16
MESH = pl.DeviceIdType.MESH
CENTRE = 9.0
RADIUS = 9.0
TRUST = 1000.0
AHEAD = 6


def iota(shape, dim):
    return lax.broadcasted_iota(jnp.int32, shape, dim)


def arrange(tiles, innovation, error, offset, cell, owner, count, send):
    blocks = innovation.shape[0]
    slots = tiles * CAP
    owners = owner[...]
    live = count[0]
    row, col = iota((blocks, blocks), 0), iota((blocks, blocks), 1)
    owners_f = owners.astype(F32)
    owners_col = jnp.sum(jnp.where(row == col, owners_f, 0.0), axis=1, keepdims=True)
    earlier = (owners_col == owners_f) & (row < col) & (row < live)
    rank = jnp.sum(jnp.where(earlier, 1.0, 0.0), axis=0, keepdims=True)
    lane = iota((1, blocks), 1)
    target = jnp.where(lane < live, owners_f * CAP + rank, -1.0)
    pick = jnp.where(iota((slots, blocks), 0).astype(F32) == target, 1.0, 0.0).astype(BF16)
    err = error[...]
    rest = jnp.concatenate(
        [innovation[...] / (err * err), offset[0], offset[1], cell[...].astype(F32)], axis=1
    )
    out = None
    for _ in range(3):
        part = rest.astype(BF16)
        term = jnp.dot(pick, part, preferred_element_type=F32)
        out = term if out is None else out + term
        rest = rest - part.astype(F32)
    for f in range(FIELDS):
        send[pl.ds(f, slots, stride=FIELDS), :] = out[:, f * LANE : (f + 1) * LANE]


def weigh(values, k, rows, cols, index, lhs, rhs):
    amount, north, east = values[0:1], values[1:2], values[2:3]
    cell = values[3:4].astype(jnp.int32)
    cell_row = lax.div(cell, cols)
    cell_col = lax.rem(cell, cols)
    part = lax.rem(cell_col, SPLIT)
    spot = iota((8, LANE), 0)
    across = jnp.where(spot == part, 1.0 - east, jnp.where(spot == part + 1, east, 0.0)) * amount
    down_at = iota((rows, LANE), 0)
    down = jnp.where(down_at == cell_row, 1.0 - north, jnp.where(down_at == cell_row + 1, north, 0.0))
    below = jnp.where(cell_row == rows - 1, north, 0.0) * across
    pieces = [down * across[c : c + 1] for c in range(PART)]
    pieces.append(jnp.concatenate([below, jnp.zeros((8, LANE), F32)], axis=0))
    second = PART * rows + 16
    for c, piece in enumerate(pieces):
        end = c * rows + piece.shape[0]
        main = piece.astype(BF16)
        lhs[k, c * rows : end, :] = main
        lhs[k, second + c * rows : second + end, :] = (piece - main.astype(F32)).astype(BF16)
    spots = index[...]
    column = lax.div(cell_col, SPLIT).astype(F32).astype(BF16)
    rhs[k] = jnp.where(spots == column, jnp.ones_like(spots), jnp.zeros_like(spots))


def weigh_group(recv, start, rows, cols, index, lhs, rhs):
    for i in range(0, GROUP * ROWS, 8):
        pair = recv[pl.ds(pl.multiple_of(start + i, 8), 8), :]
        for k in range(0, 8, FIELDS):
            weigh(pair[k : k + FIELDS], (i + k) // FIELDS, rows, cols, index, lhs, rhs)


def add_group(lhs, rhs, total):
    total[...] += lax.dot_general(
        jnp.concatenate([lhs[k] for k in range(lhs.shape[0])], axis=1),
        jnp.concatenate([rhs[k] for k in range(rhs.shape[0])], axis=1),
        (((1,), (1,)), ((), ())),
        preferred_element_type=F32,
    )


def total_shape(rows, cols):
    return (2 * (PART * rows + 16), cols // SPLIT)


def unpack(total, rows, cols, part):
    wide = cols // SPLIT
    half = rows // 2
    count = PART * rows + 16
    acc = total[0:count, :] + total[count : 2 * count, :]
    under = acc[PART * rows : PART * rows + 8]
    top = iota((8, wide), 0) == 0
    fields = []
    for c in range(PART):
        row = jnp.where(top, jnp.broadcast_to(under[c : c + 1], (8, wide)), 0.0)
        fields.append(jnp.concatenate([acc[c * rows : (c + 1) * rows], row], axis=0))
    carried = pltpu.roll(fields[SPLIT], 1, 1)
    first = iota(carried.shape, 1) == 0
    past = jnp.where(first, carried, 0.0)[:, :LANE]
    fields[0] = fields[0] + jnp.where(first, 0.0, carried)
    size = SPLIT * LANE
    source, place = iota((size, size), 0), iota((size, size), 1)
    order = jnp.where(place == SPLIT * (source % LANE) + source // LANE, 1.0, 0.0).astype(BF16)
    strips = []
    for j in range(wide // LANE):
        rest = jnp.concatenate([f[:, j * LANE : (j + 1) * LANE] for f in fields[:SPLIT]], axis=1)
        out = None
        for _ in range(3):
            piece = rest.astype(BF16)
            term = jnp.dot(piece, order, preferred_element_type=F32)
            out = term if out is None else out + term
            rest = rest - piece.astype(F32)
        strips.append(out)
    for j, out in enumerate(strips):
        at = slice(j * size, (j + 1) * size)
        part[0, 0:half, at] = out[0:half]
        part[0, half : half + 8, at] = jnp.zeros((8, size), F32)
        part[1, :, at] = out[half:]
    part[0, 0:half, cols:] = past[0:half]
    part[0, half : half + 8, cols:] = jnp.zeros((8, LANE), F32)
    part[1, :, cols:] = past[half:]


def add_up(values):
    while len(values) > 1:
        rest = values[len(values) & ~1 :]
        values = [values[i] + values[i + 1] for i in range(0, len(values) - 1, 2)] + rest
    return values[0]


def coefficients(mu):
    start = mu[0]
    mu = [m / start for m in mu]
    gram = {}
    for s in range(2 * ITERS + 1):
        for d in range(s + 1):
            gram[s, d] = 0.5 * (mu[s] + mu[d])

    def inner(a, b):
        terms = [a[i] * b[j] * gram[i + j, abs(i - j)] for i in range(len(a)) for j in range(len(b))]
        return add_up(terms)

    def operate(a):
        out = [CENTRE * v for v in a] + [None]
        for i, v in enumerate(a):
            for j, f in ((1, RADIUS),) if i == 0 else ((i + 1, RADIUS / 2), (i - 1, RADIUS / 2)):
                out[j] = f * v if out[j] is None else out[j] + f * v
        return out

    one = jnp.ones_like(start)
    field, residual, direction = [], [one], [one]
    norm = one
    worst = one
    for _ in range(ITERS):
        applied = operate(direction)
        step = norm / inner(direction, applied)
        field = [
            step * d + (field[i] if i < len(field) else 0.0) for i, d in enumerate(direction)
        ]
        residual = [
            (residual[i] if i < len(residual) else 0.0) - step * a for i, a in enumerate(applied)
        ]
        after = inner(residual, residual)
        size = add_up([jnp.abs(v) for v in residual])
        worst = jnp.maximum(worst, jnp.where(after > 0, size * size / after, 1e30))
        ratio = after / norm
        direction = [
            v + (ratio * direction[i] if i < len(direction) else 0.0) for i, v in enumerate(residual)
        ]
        norm = after
    sound = jnp.where(worst < TRUST, 1.0, 0.0)
    return field, residual, sound


def step_kernel(
    n_lat,
    n_lon,
    innovation,
    error,
    offset,
    cell,
    owner,
    count,
    land,
    inertia,
    depth,
    field_out,
    residual_out,
    forcing_out,
    sound_out,
    send,
    recv,
    lhs_a,
    rhs_a,
    lhs_b,
    rhs_b,
    index,
    total,
    part,
    got,
    mine,
    west,
    east,
    tall,
    above,
    below,
    coef,
    cond,
    basis,
    line_in,
    line_at,
    rank_in,
    rank_at,
    out_sem,
    in_sem,
    send_sem,
    recv_sem,
    line_send,
    line_recv,
    rank_send,
    rank_recv,
):
    rows, cols = land.shape
    high, wide = rows + 2 * EDGE, cols + 2 * LANE
    lat, lon, obs = lax.axis_index("lat"), lax.axis_index("lon"), lax.axis_index("obs")
    tiles = n_lat * n_lon
    ranks = 2 * n_lat
    rank = lat * 2 + obs
    quads = n_lon // GROUP
    groups = n_lat * quads

    def on_line(k):
        return {"lon": k}

    def on_rank(k):
        return {"lat": lax.div(k, 2), "obs": lax.rem(k, 2)}

    def on_tile(k):
        return {"lat": lax.div(k, n_lon), "lon": lax.rem(k, n_lon)}

    me = lat * n_lon + lon
    barrier = pltpu.get_barrier_semaphore()

    def greet_tile(d, carry):
        device = on_tile(lax.rem(me + d, tiles))
        pl.semaphore_signal(barrier, 1, device_id=device, device_id_type=MESH)
        return carry

    def greet_other(d, carry):
        device = {"lat": lax.rem(lat + d, n_lat), "obs": 1 - obs}
        pl.semaphore_signal(barrier, 1, device_id=device, device_id_type=MESH)
        return carry

    lax.fori_loop(1, tiles, greet_tile, 0)
    lax.fori_loop(0, n_lat, greet_other, 0)

    inner_rows, inner_cols = slice(EDGE, EDGE + rows), slice(LANE, LANE + cols)
    coef[0, inner_rows, inner_cols] = land[...].astype(F32) * depth[...]
    coef[1, inner_rows, inner_cols] = inertia[...]
    arrange(tiles, innovation, error, offset, cell, owner, count, send)
    pl.semaphore_wait(barrier, tiles - 1 + n_lat)

    def copy(k, src, dst, device):
        c = pltpu.make_async_remote_copy(
            src_ref=src,
            dst_ref=dst,
            send_sem=send_sem.at[k],
            recv_sem=recv_sem.at[k],
            device_id=device,
            device_id_type=MESH,
        )
        c.start()
        return c

    to_east, to_west = on_line(lax.rem(lon + 1, n_lon)), on_line(lax.rem(lon + n_lon - 1, n_lon))
    to_south, to_north = on_rank(lax.rem(rank + 1, ranks)), on_rank(lax.rem(rank + ranks - 1, ranks))
    own = pl.ds(EDGE, rows)

    coef_e = copy(1, coef.at[:, own, pl.ds(cols, LANE)], coef.at[:, own, pl.ds(0, LANE)], to_east)
    coef_w = copy(2, coef.at[:, own, pl.ds(LANE, LANE)], coef.at[:, own, pl.ds(LANE + cols, LANE)], to_west)

    quad, place = lax.div(lon, GROUP), lax.rem(lon, GROUP)

    def away(t):
        j = lax.div(t, quads)
        odd = lax.rem(j, 2)
        return lax.rem(odd * lax.div(j + 1, 2) + (1 - odd) * (n_lat - lax.div(j, 2)), n_lat)

    def rows_of(k):
        return pl.ds(k * ROWS, ROWS)

    my_group = lat * quads + quad

    def deliver(t, carry):
        to_lat = lax.rem(lat + n_lat - away(t), n_lat)
        to_quad = lax.rem(quad + quads - lax.rem(t, quads), quads)
        for d in range(GROUP):
            to_lon = to_quad * GROUP + lax.rem(place + d, GROUP)
            transfer = pltpu.make_async_remote_copy(
                src_ref=send.at[rows_of(to_lat * n_lon + to_lon), :],
                dst_ref=recv.at[rows_of(me), :],
                send_sem=out_sem,
                recv_sem=in_sem.at[my_group],
                device_id={"lat": to_lat, "lon": to_lon},
                device_id_type=MESH,
            )
            if d:
                transfer.start()
            else:
                pl.when(t > 0)(transfer.start)
        return carry

    pltpu.make_async_copy(send.at[rows_of(me), :], recv.at[rows_of(me), :], in_sem.at[my_group]).start()
    lax.fori_loop(0, min(AHEAD, groups), deliver, 0)
    total[...] = jnp.zeros_like(total)
    index[...] = iota(index.shape, 0).astype(F32).astype(BF16)
    height = GROUP * ROWS

    def group_of(t):
        from_lat = lax.rem(lat + away(t), n_lat)
        return from_lat * quads + lax.rem(quad + lax.rem(t, quads), quads)

    def await_group(t):
        g = group_of(t)
        landed = recv.at[pl.ds(pl.multiple_of(g * height, 8), height), :]
        pltpu.make_async_copy(landed, landed, in_sem.at[g]).wait()

    def weigh_next(t, lhs, rhs):
        weigh_group(recv, group_of(t) * height, 2 * rows, cols, index, lhs, rhs)

    await_group(0)
    weigh_next(0, lhs_a, rhs_a)

    def spread_two(i, carry):
        begin = jnp.minimum(2 * i + AHEAD, groups)
        lax.fori_loop(begin, jnp.minimum(begin + 2, groups), deliver, 0)
        await_group(2 * i + 1)
        weigh_next(2 * i + 1, lhs_b, rhs_b)
        add_group(lhs_a, rhs_a, total)
        await_group(2 * i + 2)
        weigh_next(2 * i + 2, lhs_a, rhs_a)
        add_group(lhs_b, rhs_b, total)
        return carry

    lax.fori_loop(0, groups // 2 - 1, spread_two, 0)
    await_group(groups - 1)
    weigh_next(groups - 1, lhs_b, rhs_b)
    add_group(lhs_a, rhs_a, total)
    add_group(lhs_b, rhs_b, total)
    gone = send.at[pl.ds(0, (tiles - 1) * ROWS), :]
    pltpu.make_async_copy(gone, gone, out_sem).wait()
    unpack(total, 2 * rows, cols, part)

    coef_e.wait_recv()
    coef_w.wait_recv()
    coef_s = copy(5, coef.at[:, pl.ds(rows, EDGE), :], coef.at[:, pl.ds(0, EDGE), :], to_south)
    coef_n = copy(6, coef.at[:, pl.ds(EDGE, EDGE), :], coef.at[:, pl.ds(EDGE + rows, EDGE), :], to_north)
    pair = copy(0, part.at[1 - obs], got, {"obs": 1 - obs})
    pair.wait_recv()
    mine[...] = part[obs] + got[...]
    mine_e = copy(3, mine.at[:, pl.ds(cols - LANE, 2 * LANE)], west, to_east)
    mine_w = copy(4, mine.at[:, pl.ds(0, LANE)], east, to_west)
    mine_e.wait_recv()
    mine_w.wait_recv()
    tall[:, 0:LANE] = west[:, 0:LANE]
    tall[:, LANE : 2 * LANE] = mine[:, 0:LANE] + west[:, LANE:]
    tall[:, 2 * LANE : LANE + cols] = mine[:, LANE:cols]
    tall[:, LANE + cols :] = mine[:, cols:] + east[...]
    tall_s = copy(7, tall.at[pl.ds(rows - EDGE, 2 * EDGE), :], above, to_south)
    tall_n = copy(8, tall.at[pl.ds(0, EDGE), :], below, to_north)
    coef_s.wait_recv()
    coef_n.wait_recv()
    conduct = coef[0]
    north = jnp.sqrt(conduct * pltpu.roll(conduct, 1, 0))
    south = pltpu.roll(north, high - 1, 0)
    left = jnp.sqrt(conduct * pltpu.roll(conduct, 1, 1))
    right = pltpu.roll(left, wide - 1, 1)
    cond[0] = (coef[1] + north + south + left + right - CENTRE) * (1.0 / RADIUS)
    cond[1] = north * (1.0 / RADIUS)
    cond[2] = south * (1.0 / RADIUS)
    cond[3] = left * (1.0 / RADIUS)
    cond[4] = right * (1.0 / RADIUS)
    tall_s.wait_recv()
    tall_n.wait_recv()
    ocean = coef[0] > 0
    raw = jnp.concatenate(
        [
            above[0:EDGE, :],
            tall[0:EDGE, :] + above[EDGE:, :],
            tall[EDGE:rows, :],
            below[...] + tall[rows:, :],
        ],
        axis=0,
    )
    basis[0] = jnp.where(ocean, raw, 0.0)
    forcing_out[...] = basis[0, inner_rows, inner_cols]

    def operate(v):
        return (
            cond[0] * v
            - cond[1] * pltpu.roll(v, 1, 0)
            - cond[2] * pltpu.roll(v, high - 1, 0)
            - cond[3] * pltpu.roll(v, 1, 1)
            - cond[4] * pltpu.roll(v, wide - 1, 1)
        )

    for k in range(ITERS):
        after = operate(basis[k])
        basis[k + 1] = after if k == 0 else 2.0 * after - basis[k - 1]

    def dot(i, j):
        pieces = []
        for a in range(EDGE, EDGE + rows, 8):
            for b in range(LANE, LANE + cols, LANE):
                pieces.append(basis[i, a : a + 8, b : b + LANE] * basis[j, a : a + 8, b : b + LANE])
        return jnp.sum(add_up(pieces), axis=0, keepdims=True)

    pairs = [(k // 2, (k + 1) // 2) for k in range(2 * ITERS + 1)]
    sums = [dot(i, j) for i, j in pairs]
    stack = jnp.concatenate(sums + [jnp.zeros((16 - len(sums), LANE), F32)], axis=0)
    column = jnp.sum(stack, axis=1, keepdims=True)
    diag = iota((16, LANE), 0) == iota((16, LANE), 1)
    line_in[...] = jnp.sum(jnp.where(diag, column, 0.0), axis=0, keepdims=True)

    def share(count, me, device, value, at, s_sem, r_sem):
        def copy_of(slot, k, target):
            return pltpu.make_async_remote_copy(
                src_ref=value,
                dst_ref=at.at[slot],
                send_sem=s_sem.at[k],
                recv_sem=r_sem.at[slot],
                device_id=device(target),
                device_id_type=MESH,
            )

        half = count // 2
        offsets = [half] + [half + s * k for k in range(1, half) for s in (1, -1)]
        for d in offsets:
            copy_of(me, d, lax.rem(me + d, count)).start()
        at[me] = value[...]
        for d in reversed(offsets):
            copy_of(lax.rem(me + count - d, count), d, lax.rem(me + d, count)).wait_recv()
        for d in offsets:
            copy_of(me, d, lax.rem(me + d, count)).wait_send()
        return add_up([at[k] for k in range(count)])

    rank_in[...] = share(n_lon, lon, on_line, line_in, line_at, line_send, line_recv)
    sums = share(ranks, rank, on_rank, rank_in, rank_at, rank_send, rank_recv)
    lane = iota((1, LANE), 1)
    raw_sums = [
        jnp.sum(jnp.where(lane == k, sums, 0.0), axis=1, keepdims=True) for k in range(2 * ITERS + 1)
    ]
    mu = [
        raw_sums[k] if k < 2 else 2.0 * raw_sums[k] - raw_sums[k % 2] for k in range(2 * ITERS + 1)
    ]
    field, residual, sound = coefficients(mu)
    views = [basis[k, inner_rows, inner_cols] for k in range(ITERS + 1)]
    field_out[...] = add_up([c * v for c, v in zip(field, views)])
    residual_out[...] = add_up([c * v for c, v in zip(residual, views)])
    sound_out[...] = jnp.broadcast_to(sound, (1, LANE))
    for c in (pair, coef_e, coef_w, mine_e, mine_w, coef_s, coef_n, tall_s, tall_n):
        c.wait_send()


def step(n_lat, n_lon, innovation, error, offset, cell, owner, count, land, inertia, depth):
    rows, cols = land.shape
    high, wide = rows + 2 * EDGE, cols + 2 * LANE
    own = jax.ShapeDtypeStruct((rows, cols), F32)
    vmem = pl.BlockSpec(memory_space=pltpu.VMEM)
    ranks = 2 * n_lat
    tiles = n_lat * n_lon
    groups = tiles // GROUP
    tall = total_shape(2 * rows, cols)
    deep = GROUP * CAP
    return pl.pallas_call(
        functools.partial(step_kernel, n_lat, n_lon),
        out_shape=(own, own, own, jax.ShapeDtypeStruct((1, LANE), F32)),
        in_specs=[vmem] * 5 + [pl.BlockSpec(memory_space=pltpu.SMEM)] + [vmem] * 3,
        out_specs=(vmem,) * 4,
        scratch_shapes=[
            pltpu.VMEM((tiles * ROWS, LANE), F32),
            pltpu.VMEM((tiles * ROWS, LANE), F32),
            pltpu.VMEM((deep, tall[0], LANE), BF16),
            pltpu.VMEM((deep, tall[1], LANE), BF16),
            pltpu.VMEM((deep, tall[0], LANE), BF16),
            pltpu.VMEM((deep, tall[1], LANE), BF16),
            pltpu.VMEM((tall[1], LANE), BF16),
            pltpu.VMEM(tall, F32),
            pltpu.VMEM((2, rows + EDGE, cols + LANE), F32),
            pltpu.VMEM((rows + EDGE, cols + LANE), F32),
            pltpu.VMEM((rows + EDGE, cols + LANE), F32),
            pltpu.VMEM((rows + EDGE, 2 * LANE), F32),
            pltpu.VMEM((rows + EDGE, LANE), F32),
            pltpu.VMEM((rows + EDGE, wide), F32),
            pltpu.VMEM((2 * EDGE, wide), F32),
            pltpu.VMEM((EDGE, wide), F32),
            pltpu.VMEM((2, high, wide), F32),
            pltpu.VMEM((5, high, wide), F32),
            pltpu.VMEM((ITERS + 1, high, wide), F32),
            pltpu.VMEM((1, LANE), F32),
            pltpu.VMEM((n_lon, 1, LANE), F32),
            pltpu.VMEM((1, LANE), F32),
            pltpu.VMEM((ranks, 1, LANE), F32),
            pltpu.SemaphoreType.DMA,
            pltpu.SemaphoreType.DMA((groups,)),
            pltpu.SemaphoreType.DMA((9,)),
            pltpu.SemaphoreType.DMA((9,)),
            pltpu.SemaphoreType.DMA((n_lon,)),
            pltpu.SemaphoreType.DMA((n_lon,)),
            pltpu.SemaphoreType.DMA((ranks,)),
            pltpu.SemaphoreType.DMA((ranks,)),
        ],
        compiler_params=pltpu.CompilerParams(collective_id=1, has_side_effects=True),
    )(innovation, error, offset, cell, owner, count, land, inertia, depth)


def shifted(value, axis, steps):
    count = lax.axis_size(axis)
    return lax.ppermute(value, axis, [(i, (i + steps) % count) for i in range(count)])


def border(block):
    for axis, dim in ((("lat", "obs"), 0), ("lon", 1)):
        size = block.shape[dim]
        low = shifted(lax.slice_in_dim(block, size - 1, size, axis=dim), axis, 1)
        high = shifted(lax.slice_in_dim(block, 0, 1, axis=dim), axis, -1)
        block = jnp.concatenate([low, block, high], axis=dim)
    return block


def stepwise(sound, field, residual, forcing, land, own, sea):
    def whole(value):
        return lax.psum(jnp.sum(value), ("lat", "lon", "obs"))

    def step(_, state):
        (field, residual, direction, before), depth, inertia = lax.optimization_barrier(
            (state, sea, own)
        )
        conduct = land.astype(F32) * depth
        padded = border(conduct)
        north = jnp.sqrt(conduct * padded[:-2, 1:-1])
        south = jnp.sqrt(conduct * padded[2:, 1:-1])
        west = jnp.sqrt(conduct * padded[1:-1, :-2])
        east = jnp.sqrt(conduct * padded[1:-1, 2:])
        diagonal = inertia + north + south + west + east
        norm = whole(residual * residual)
        direction = residual + norm / before * direction
        outer = border(direction)
        applied = (
            diagonal * direction
            - north * outer[:-2, 1:-1]
            - south * outer[2:, 1:-1]
            - west * outer[1:-1, :-2]
            - east * outer[1:-1, 2:]
        )
        size = norm / whole(direction * applied)
        return field + size * direction, residual - size * applied, direction, norm

    state = (
        jnp.where(sound, field, 0.0),
        jnp.where(sound, residual, forcing),
        jnp.zeros_like(forcing),
        jnp.float32(1.0),
    )
    return lax.fori_loop(0, jnp.where(sound, 0, ITERS), step, state)[:2]


def body(n_lat, n_lon, *inputs):
    land, inertia, depth = inputs[-3:]
    field, residual, forcing, sound = step(n_lat, n_lon, *inputs)
    return stepwise(sound[0, 0] > 0.5, field, residual, forcing, land, inertia, depth)


def solution(mesh):
    split = ("lat", "lon", "obs")
    grid = P(("lat", "obs"), "lon")
    return jax.shard_map(
        functools.partial(body, mesh.shape["lat"], mesh.shape["lon"]),
        mesh=mesh,
        in_specs=(
            P(split, None),
            P(split, None),
            P(None, split, None),
            P(split, None),
            P(split, None),
            P(split),
            grid,
            grid,
            grid,
        ),
        out_specs=(grid, grid),
        check_vma=False,
    )
```

```python
import functools

import jax
import jax.numpy as jnp
from jax import lax
from jax.experimental import pallas as pl
from jax.experimental.pallas import tpu as pltpu
from jax.sharding import PartitionSpec as P

ITERS = 5
CAP = 3
FIELDS = 4
ROWS = CAP * FIELDS
GROUP = 4
SPLIT = 4
PART = SPLIT + 1
LANE = 128
EDGE = 8
F32 = jnp.float32
BF16 = jnp.bfloat16
MESH = pl.DeviceIdType.MESH
CENTRE = 9.0
RADIUS = 9.0
TRUST = 1000.0
AHEAD = 12


def iota(shape, dim):
    return lax.broadcasted_iota(jnp.int32, shape, dim)


def arrange(tiles, innovation, error, offset, cell, owner, count, send):
    blocks = innovation.shape[0]
    slots = tiles * CAP
    owners = owner[...]
    live = count[0]
    row, col = iota((blocks, blocks), 0), iota((blocks, blocks), 1)
    owners_f = owners.astype(F32)
    owners_col = jnp.sum(jnp.where(row == col, owners_f, 0.0), axis=1, keepdims=True)
    earlier = (owners_col == owners_f) & (row < col) & (row < live)
    rank = jnp.sum(jnp.where(earlier, 1.0, 0.0), axis=0, keepdims=True)
    lane = iota((1, blocks), 1)
    target = jnp.where(lane < live, owners_f * CAP + rank, -1.0)
    pick = jnp.where(iota((slots, blocks), 0).astype(F32) == target, 1.0, 0.0).astype(BF16)
    err = error[...]
    rest = jnp.concatenate(
        [innovation[...] / (err * err), offset[0], offset[1], cell[...].astype(F32)], axis=1
    )
    out = None
    for _ in range(3):
        part = rest.astype(BF16)
        term = jnp.dot(pick, part, preferred_element_type=F32)
        out = term if out is None else out + term
        rest = rest - part.astype(F32)
    for f in range(FIELDS):
        send[pl.ds(f, slots, stride=FIELDS), :] = out[:, f * LANE : (f + 1) * LANE]


def weigh(values, k, rows, cols, index, lhs, rhs):
    amount, north, east = values[0:1], values[1:2], values[2:3]
    cell = values[3:4].astype(jnp.int32)
    cell_row = lax.div(cell, cols)
    cell_col = lax.rem(cell, cols)
    part = lax.rem(cell_col, SPLIT)
    spot = iota((8, LANE), 0)
    across = jnp.where(spot == part, 1.0 - east, jnp.where(spot == part + 1, east, 0.0)) * amount
    down_at = iota((rows, LANE), 0)
    down = jnp.where(down_at == cell_row, 1.0 - north, jnp.where(down_at == cell_row + 1, north, 0.0))
    below = jnp.where(cell_row == rows - 1, north, 0.0) * across
    pieces = [down * across[c : c + 1] for c in range(PART)]
    pieces.append(jnp.concatenate([below, jnp.zeros((8, LANE), F32)], axis=0))
    second = PART * rows + 16
    for c, piece in enumerate(pieces):
        end = c * rows + piece.shape[0]
        main = piece.astype(BF16)
        lhs[k, c * rows : end, :] = main
        lhs[k, second + c * rows : second + end, :] = (piece - main.astype(F32)).astype(BF16)
    spots = index[...]
    column = lax.div(cell_col, SPLIT).astype(F32).astype(BF16)
    rhs[k] = jnp.where(spots == column, jnp.ones_like(spots), jnp.zeros_like(spots))


def weigh_group(recv, start, rows, cols, index, lhs, rhs):
    for i in range(0, GROUP * ROWS, 8):
        pair = recv[pl.ds(pl.multiple_of(start + i, 8), 8), :]
        for k in range(0, 8, FIELDS):
            weigh(pair[k : k + FIELDS], (i + k) // FIELDS, rows, cols, index, lhs, rhs)


def add_group(lhs, rhs, total):
    total[...] += lax.dot_general(
        jnp.concatenate([lhs[k] for k in range(lhs.shape[0])], axis=1),
        jnp.concatenate([rhs[k] for k in range(rhs.shape[0])], axis=1),
        (((1,), (1,)), ((), ())),
        preferred_element_type=F32,
    )


def total_shape(rows, cols):
    return (2 * (PART * rows + 16), cols // SPLIT)


def unpack(total, rows, cols, part):
    wide = cols // SPLIT
    half = rows // 2
    count = PART * rows + 16
    acc = total[0:count, :] + total[count : 2 * count, :]
    under = acc[PART * rows : PART * rows + 8]
    top = iota((8, wide), 0) == 0
    fields = []
    for c in range(PART):
        row = jnp.where(top, jnp.broadcast_to(under[c : c + 1], (8, wide)), 0.0)
        fields.append(jnp.concatenate([acc[c * rows : (c + 1) * rows], row], axis=0))
    carried = pltpu.roll(fields[SPLIT], 1, 1)
    first = iota(carried.shape, 1) == 0
    past = jnp.where(first, carried, 0.0)[:, :LANE]
    fields[0] = fields[0] + jnp.where(first, 0.0, carried)
    size = SPLIT * LANE
    source, place = iota((size, size), 0), iota((size, size), 1)
    order = jnp.where(place == SPLIT * (source % LANE) + source // LANE, 1.0, 0.0).astype(BF16)
    strips = []
    for j in range(wide // LANE):
        rest = jnp.concatenate([f[:, j * LANE : (j + 1) * LANE] for f in fields[:SPLIT]], axis=1)
        out = None
        for _ in range(3):
            piece = rest.astype(BF16)
            term = jnp.dot(piece, order, preferred_element_type=F32)
            out = term if out is None else out + term
            rest = rest - piece.astype(F32)
        strips.append(out)
    for j, out in enumerate(strips):
        at = slice(j * size, (j + 1) * size)
        part[0, 0:half, at] = out[0:half]
        part[0, half : half + 8, at] = jnp.zeros((8, size), F32)
        part[1, :, at] = out[half:]
    part[0, 0:half, cols:] = past[0:half]
    part[0, half : half + 8, cols:] = jnp.zeros((8, LANE), F32)
    part[1, :, cols:] = past[half:]


def add_up(values):
    while len(values) > 1:
        rest = values[len(values) & ~1 :]
        values = [values[i] + values[i + 1] for i in range(0, len(values) - 1, 2)] + rest
    return values[0]


def coefficients(mu):
    start = mu[0]
    mu = [m / start for m in mu]
    gram = {}
    for s in range(2 * ITERS + 1):
        for d in range(s + 1):
            gram[s, d] = 0.5 * (mu[s] + mu[d])

    def inner(a, b):
        terms = [a[i] * b[j] * gram[i + j, abs(i - j)] for i in range(len(a)) for j in range(len(b))]
        return add_up(terms)

    def operate(a):
        out = [CENTRE * v for v in a] + [None]
        for i, v in enumerate(a):
            for j, f in ((1, RADIUS),) if i == 0 else ((i + 1, RADIUS / 2), (i - 1, RADIUS / 2)):
                out[j] = f * v if out[j] is None else out[j] + f * v
        return out

    one = jnp.ones_like(start)
    field, residual, direction = [], [one], [one]
    norm = one
    worst = one
    for _ in range(ITERS):
        applied = operate(direction)
        step = norm / inner(direction, applied)
        field = [
            step * d + (field[i] if i < len(field) else 0.0) for i, d in enumerate(direction)
        ]
        residual = [
            (residual[i] if i < len(residual) else 0.0) - step * a for i, a in enumerate(applied)
        ]
        after = inner(residual, residual)
        size = add_up([jnp.abs(v) for v in residual])
        worst = jnp.maximum(worst, jnp.where(after > 0, size * size / after, 1e30))
        ratio = after / norm
        direction = [
            v + (ratio * direction[i] if i < len(direction) else 0.0) for i, v in enumerate(residual)
        ]
        norm = after
    sound = jnp.where(worst < TRUST, 1.0, 0.0)
    return field, residual, sound


def step_kernel(
    n_lat,
    n_lon,
    innovation,
    error,
    offset,
    cell,
    owner,
    count,
    land,
    inertia,
    depth,
    field_out,
    residual_out,
    forcing_out,
    sound_out,
    send,
    recv,
    lhs_a,
    rhs_a,
    lhs_b,
    rhs_b,
    index,
    total,
    part,
    got,
    mine,
    west,
    east,
    tall,
    above,
    below,
    coef,
    cond,
    basis,
    line_in,
    line_at,
    rank_in,
    rank_at,
    out_sem,
    in_sem,
    send_sem,
    recv_sem,
    line_send,
    line_recv,
    rank_send,
    rank_recv,
):
    rows, cols = land.shape
    high, wide = rows + 2 * EDGE, cols + 2 * LANE
    lat, lon, obs = lax.axis_index("lat"), lax.axis_index("lon"), lax.axis_index("obs")
    tiles = n_lat * n_lon
    ranks = 2 * n_lat
    rank = lat * 2 + obs
    quads = n_lon // GROUP
    groups = n_lat * quads

    def on_line(k):
        return {"lon": k}

    def on_rank(k):
        return {"lat": lax.div(k, 2), "obs": lax.rem(k, 2)}

    def on_tile(k):
        return {"lat": lax.div(k, n_lon), "lon": lax.rem(k, n_lon)}

    me = lat * n_lon + lon
    barrier = pltpu.get_barrier_semaphore()

    def greet_tile(d, carry):
        device = on_tile(lax.rem(me + d, tiles))
        pl.semaphore_signal(barrier, 1, device_id=device, device_id_type=MESH)
        return carry

    def greet_other(d, carry):
        device = {"lat": lax.rem(lat + d, n_lat), "obs": 1 - obs}
        pl.semaphore_signal(barrier, 1, device_id=device, device_id_type=MESH)
        return carry

    lax.fori_loop(1, tiles, greet_tile, 0)
    lax.fori_loop(0, n_lat, greet_other, 0)

    inner_rows, inner_cols = slice(EDGE, EDGE + rows), slice(LANE, LANE + cols)
    coef[0, inner_rows, inner_cols] = land[...].astype(F32) * depth[...]
    coef[1, inner_rows, inner_cols] = inertia[...]
    arrange(tiles, innovation, error, offset, cell, owner, count, send)
    pl.semaphore_wait(barrier, tiles - 1 + n_lat)

    def copy(k, src, dst, device):
        c = pltpu.make_async_remote_copy(
            src_ref=src,
            dst_ref=dst,
            send_sem=send_sem.at[k],
            recv_sem=recv_sem.at[k],
            device_id=device,
            device_id_type=MESH,
        )
        c.start()
        return c

    to_east, to_west = on_line(lax.rem(lon + 1, n_lon)), on_line(lax.rem(lon + n_lon - 1, n_lon))
    to_south, to_north = on_rank(lax.rem(rank + 1, ranks)), on_rank(lax.rem(rank + ranks - 1, ranks))
    own = pl.ds(EDGE, rows)

    coef_e = copy(1, coef.at[:, own, pl.ds(cols, LANE)], coef.at[:, own, pl.ds(0, LANE)], to_east)
    coef_w = copy(2, coef.at[:, own, pl.ds(LANE, LANE)], coef.at[:, own, pl.ds(LANE + cols, LANE)], to_west)

    quad, place = lax.div(lon, GROUP), lax.rem(lon, GROUP)

    def away(t):
        j = lax.div(t, quads)
        odd = lax.rem(j, 2)
        return lax.rem(odd * lax.div(j + 1, 2) + (1 - odd) * (n_lat - lax.div(j, 2)), n_lat)

    def rows_of(k):
        return pl.ds(k * ROWS, ROWS)

    my_group = lat * quads + quad

    def deliver(t, carry):
        to_lat = lax.rem(lat + n_lat - away(t), n_lat)
        to_quad = lax.rem(quad + quads - lax.rem(t, quads), quads)
        for d in range(GROUP):
            to_lon = to_quad * GROUP + lax.rem(place + d, GROUP)
            transfer = pltpu.make_async_remote_copy(
                src_ref=send.at[rows_of(to_lat * n_lon + to_lon), :],
                dst_ref=recv.at[rows_of(me), :],
                send_sem=out_sem,
                recv_sem=in_sem.at[my_group],
                device_id={"lat": to_lat, "lon": to_lon},
                device_id_type=MESH,
            )
            if d:
                transfer.start()
            else:
                pl.when(t > 0)(transfer.start)
        return carry

    pltpu.make_async_copy(send.at[rows_of(me), :], recv.at[rows_of(me), :], in_sem.at[my_group]).start()
    lax.fori_loop(0, min(AHEAD, groups), deliver, 0)
    total[...] = jnp.zeros_like(total)
    index[...] = iota(index.shape, 0).astype(F32).astype(BF16)
    height = GROUP * ROWS

    def group_of(t):
        from_lat = lax.rem(lat + away(t), n_lat)
        return from_lat * quads + lax.rem(quad + lax.rem(t, quads), quads)

    def await_group(t):
        g = group_of(t)
        landed = recv.at[pl.ds(pl.multiple_of(g * height, 8), height), :]
        pltpu.make_async_copy(landed, landed, in_sem.at[g]).wait()

    def weigh_next(t, lhs, rhs):
        weigh_group(recv, group_of(t) * height, 2 * rows, cols, index, lhs, rhs)

    await_group(0)
    weigh_next(0, lhs_a, rhs_a)

    def spread_two(i, carry):
        begin = jnp.minimum(2 * i + AHEAD, groups)
        lax.fori_loop(begin, jnp.minimum(begin + 2, groups), deliver, 0)
        await_group(2 * i + 1)
        weigh_next(2 * i + 1, lhs_b, rhs_b)
        add_group(lhs_a, rhs_a, total)
        await_group(2 * i + 2)
        weigh_next(2 * i + 2, lhs_a, rhs_a)
        add_group(lhs_b, rhs_b, total)
        return carry

    lax.fori_loop(0, groups // 2 - 1, spread_two, 0)
    await_group(groups - 1)
    weigh_next(groups - 1, lhs_b, rhs_b)
    add_group(lhs_a, rhs_a, total)
    add_group(lhs_b, rhs_b, total)
    gone = send.at[pl.ds(0, (tiles - 1) * ROWS), :]
    pltpu.make_async_copy(gone, gone, out_sem).wait()
    unpack(total, 2 * rows, cols, part)

    coef_e.wait_recv()
    coef_w.wait_recv()
    coef_s = copy(5, coef.at[:, pl.ds(rows, EDGE), :], coef.at[:, pl.ds(0, EDGE), :], to_south)
    coef_n = copy(6, coef.at[:, pl.ds(EDGE, EDGE), :], coef.at[:, pl.ds(EDGE + rows, EDGE), :], to_north)
    pair = copy(0, part.at[1 - obs], got, {"obs": 1 - obs})
    pair.wait_recv()
    mine[...] = part[obs] + got[...]
    mine_e = copy(3, mine.at[:, pl.ds(cols - LANE, 2 * LANE)], west, to_east)
    mine_w = copy(4, mine.at[:, pl.ds(0, LANE)], east, to_west)
    mine_e.wait_recv()
    mine_w.wait_recv()
    tall[:, 0:LANE] = west[:, 0:LANE]
    tall[:, LANE : 2 * LANE] = mine[:, 0:LANE] + west[:, LANE:]
    tall[:, 2 * LANE : LANE + cols] = mine[:, LANE:cols]
    tall[:, LANE + cols :] = mine[:, cols:] + east[...]
    tall_s = copy(7, tall.at[pl.ds(rows - EDGE, 2 * EDGE), :], above, to_south)
    tall_n = copy(8, tall.at[pl.ds(0, EDGE), :], below, to_north)
    coef_s.wait_recv()
    coef_n.wait_recv()
    conduct = coef[0]
    north = jnp.sqrt(conduct * pltpu.roll(conduct, 1, 0))
    south = pltpu.roll(north, high - 1, 0)
    left = jnp.sqrt(conduct * pltpu.roll(conduct, 1, 1))
    right = pltpu.roll(left, wide - 1, 1)
    cond[0] = (coef[1] + north + south + left + right - CENTRE) * (1.0 / RADIUS)
    cond[1] = north * (1.0 / RADIUS)
    cond[2] = south * (1.0 / RADIUS)
    cond[3] = left * (1.0 / RADIUS)
    cond[4] = right * (1.0 / RADIUS)
    tall_s.wait_recv()
    tall_n.wait_recv()
    ocean = coef[0] > 0
    raw = jnp.concatenate(
        [
            above[0:EDGE, :],
            tall[0:EDGE, :] + above[EDGE:, :],
            tall[EDGE:rows, :],
            below[...] + tall[rows:, :],
        ],
        axis=0,
    )
    basis[0] = jnp.where(ocean, raw, 0.0)
    forcing_out[...] = basis[0, inner_rows, inner_cols]

    def operate(v):
        return (
            cond[0] * v
            - cond[1] * pltpu.roll(v, 1, 0)
            - cond[2] * pltpu.roll(v, high - 1, 0)
            - cond[3] * pltpu.roll(v, 1, 1)
            - cond[4] * pltpu.roll(v, wide - 1, 1)
        )

    for k in range(ITERS):
        after = operate(basis[k])
        basis[k + 1] = after if k == 0 else 2.0 * after - basis[k - 1]

    def dot(i, j):
        pieces = []
        for a in range(EDGE, EDGE + rows, 8):
            for b in range(LANE, LANE + cols, LANE):
                pieces.append(basis[i, a : a + 8, b : b + LANE] * basis[j, a : a + 8, b : b + LANE])
        return jnp.sum(add_up(pieces), axis=0, keepdims=True)

    pairs = [(k // 2, (k + 1) // 2) for k in range(2 * ITERS + 1)]
    sums = [dot(i, j) for i, j in pairs]
    stack = jnp.concatenate(sums + [jnp.zeros((16 - len(sums), LANE), F32)], axis=0)
    column = jnp.sum(stack, axis=1, keepdims=True)
    diag = iota((16, LANE), 0) == iota((16, LANE), 1)
    line_in[...] = jnp.sum(jnp.where(diag, column, 0.0), axis=0, keepdims=True)

    def share(count, me, device, value, at, s_sem, r_sem):
        def copy_of(slot, k, target):
            return pltpu.make_async_remote_copy(
                src_ref=value,
                dst_ref=at.at[slot],
                send_sem=s_sem.at[k],
                recv_sem=r_sem.at[slot],
                device_id=device(target),
                device_id_type=MESH,
            )

        half = count // 2
        offsets = [half] + [half + s * k for k in range(1, half) for s in (1, -1)]
        for d in offsets:
            copy_of(me, d, lax.rem(me + d, count)).start()
        at[me] = value[...]
        for d in reversed(offsets):
            copy_of(lax.rem(me + count - d, count), d, lax.rem(me + d, count)).wait_recv()
        for d in offsets:
            copy_of(me, d, lax.rem(me + d, count)).wait_send()
        return add_up([at[k] for k in range(count)])

    rank_in[...] = share(n_lon, lon, on_line, line_in, line_at, line_send, line_recv)
    sums = share(ranks, rank, on_rank, rank_in, rank_at, rank_send, rank_recv)
    lane = iota((1, LANE), 1)
    raw_sums = [
        jnp.sum(jnp.where(lane == k, sums, 0.0), axis=1, keepdims=True) for k in range(2 * ITERS + 1)
    ]
    mu = [
        raw_sums[k] if k < 2 else 2.0 * raw_sums[k] - raw_sums[k % 2] for k in range(2 * ITERS + 1)
    ]
    field, residual, sound = coefficients(mu)
    views = [basis[k, inner_rows, inner_cols] for k in range(ITERS + 1)]
    field_out[...] = add_up([c * v for c, v in zip(field, views)])
    residual_out[...] = add_up([c * v for c, v in zip(residual, views)])
    sound_out[...] = jnp.broadcast_to(sound, (1, LANE))
    for c in (pair, coef_e, coef_w, mine_e, mine_w, coef_s, coef_n, tall_s, tall_n):
        c.wait_send()


def step(n_lat, n_lon, innovation, error, offset, cell, owner, count, land, inertia, depth):
    rows, cols = land.shape
    high, wide = rows + 2 * EDGE, cols + 2 * LANE
    own = jax.ShapeDtypeStruct((rows, cols), F32)
    vmem = pl.BlockSpec(memory_space=pltpu.VMEM)
    ranks = 2 * n_lat
    tiles = n_lat * n_lon
    groups = tiles // GROUP
    tall = total_shape(2 * rows, cols)
    deep = GROUP * CAP
    return pl.pallas_call(
        functools.partial(step_kernel, n_lat, n_lon),
        out_shape=(own, own, own, jax.ShapeDtypeStruct((1, LANE), F32)),
        in_specs=[vmem] * 5 + [pl.BlockSpec(memory_space=pltpu.SMEM)] + [vmem] * 3,
        out_specs=(vmem,) * 4,
        scratch_shapes=[
            pltpu.VMEM((tiles * ROWS, LANE), F32),
            pltpu.VMEM((tiles * ROWS, LANE), F32),
            pltpu.VMEM((deep, tall[0], LANE), BF16),
            pltpu.VMEM((deep, tall[1], LANE), BF16),
            pltpu.VMEM((deep, tall[0], LANE), BF16),
            pltpu.VMEM((deep, tall[1], LANE), BF16),
            pltpu.VMEM((tall[1], LANE), BF16),
            pltpu.VMEM(tall, F32),
            pltpu.VMEM((2, rows + EDGE, cols + LANE), F32),
            pltpu.VMEM((rows + EDGE, cols + LANE), F32),
            pltpu.VMEM((rows + EDGE, cols + LANE), F32),
            pltpu.VMEM((rows + EDGE, 2 * LANE), F32),
            pltpu.VMEM((rows + EDGE, LANE), F32),
            pltpu.VMEM((rows + EDGE, wide), F32),
            pltpu.VMEM((2 * EDGE, wide), F32),
            pltpu.VMEM((EDGE, wide), F32),
            pltpu.VMEM((2, high, wide), F32),
            pltpu.VMEM((5, high, wide), F32),
            pltpu.VMEM((ITERS + 1, high, wide), F32),
            pltpu.VMEM((1, LANE), F32),
            pltpu.VMEM((n_lon, 1, LANE), F32),
            pltpu.VMEM((1, LANE), F32),
            pltpu.VMEM((ranks, 1, LANE), F32),
            pltpu.SemaphoreType.DMA,
            pltpu.SemaphoreType.DMA((groups,)),
            pltpu.SemaphoreType.DMA((9,)),
            pltpu.SemaphoreType.DMA((9,)),
            pltpu.SemaphoreType.DMA((n_lon,)),
            pltpu.SemaphoreType.DMA((n_lon,)),
            pltpu.SemaphoreType.DMA((ranks,)),
            pltpu.SemaphoreType.DMA((ranks,)),
        ],
        compiler_params=pltpu.CompilerParams(collective_id=1, has_side_effects=True),
    )(innovation, error, offset, cell, owner, count, land, inertia, depth)


def shifted(value, axis, steps):
    count = lax.axis_size(axis)
    return lax.ppermute(value, axis, [(i, (i + steps) % count) for i in range(count)])


def border(block):
    for axis, dim in ((("lat", "obs"), 0), ("lon", 1)):
        size = block.shape[dim]
        low = shifted(lax.slice_in_dim(block, size - 1, size, axis=dim), axis, 1)
        high = shifted(lax.slice_in_dim(block, 0, 1, axis=dim), axis, -1)
        block = jnp.concatenate([low, block, high], axis=dim)
    return block


def stepwise(sound, field, residual, forcing, land, own, sea):
    def whole(value):
        return lax.psum(jnp.sum(value), ("lat", "lon", "obs"))

    def step(_, state):
        (field, residual, direction, before), depth, inertia = lax.optimization_barrier(
            (state, sea, own)
        )
        conduct = land.astype(F32) * depth
        padded = border(conduct)
        north = jnp.sqrt(conduct * padded[:-2, 1:-1])
        south = jnp.sqrt(conduct * padded[2:, 1:-1])
        west = jnp.sqrt(conduct * padded[1:-1, :-2])
        east = jnp.sqrt(conduct * padded[1:-1, 2:])
        diagonal = inertia + north + south + west + east
        norm = whole(residual * residual)
        direction = residual + norm / before * direction
        outer = border(direction)
        applied = (
            diagonal * direction
            - north * outer[:-2, 1:-1]
            - south * outer[2:, 1:-1]
            - west * outer[1:-1, :-2]
            - east * outer[1:-1, 2:]
        )
        size = norm / whole(direction * applied)
        return field + size * direction, residual - size * applied, direction, norm

    state = (
        jnp.where(sound, field, 0.0),
        jnp.where(sound, residual, forcing),
        jnp.zeros_like(forcing),
        jnp.float32(1.0),
    )
    return lax.fori_loop(0, jnp.where(sound, 0, ITERS), step, state)[:2]


def body(n_lat, n_lon, *inputs):
    land, inertia, depth = inputs[-3:]
    field, residual, forcing, sound = step(n_lat, n_lon, *inputs)
    return stepwise(sound[0, 0] > 0.5, field, residual, forcing, land, inertia, depth)


def solution(mesh):
    split = ("lat", "lon", "obs")
    grid = P(("lat", "obs"), "lon")
    return jax.shard_map(
        functools.partial(body, mesh.shape["lat"], mesh.shape["lon"]),
        mesh=mesh,
        in_specs=(
            P(split, None),
            P(split, None),
            P(None, split, None),
            P(split, None),
            P(split, None),
            P(split),
            grid,
            grid,
            grid,
        ),
        out_specs=(grid, grid),
        check_vma=False,
    )
```

```python
import functools

import jax
import jax.numpy as jnp
from jax import lax
from jax.experimental import pallas as pl
from jax.experimental.pallas import tpu as pltpu
from jax.sharding import PartitionSpec as P

ITERS = 5
CAP = 3
FIELDS = 4
ROWS = CAP * FIELDS
GROUP = 8
SPLIT = 4
PART = SPLIT + 1
LANE = 128
EDGE = 8
F32 = jnp.float32
BF16 = jnp.bfloat16
MESH = pl.DeviceIdType.MESH
CENTRE = 9.0
RADIUS = 9.0
TRUST = 1000.0
AHEAD = 6


def iota(shape, dim):
    return lax.broadcasted_iota(jnp.int32, shape, dim)


def arrange(tiles, innovation, error, offset, cell, owner, count, send):
    blocks = innovation.shape[0]
    slots = tiles * CAP
    owners = owner[...]
    live = count[0]
    row, col = iota((blocks, blocks), 0), iota((blocks, blocks), 1)
    owners_f = owners.astype(F32)
    owners_col = jnp.sum(jnp.where(row == col, owners_f, 0.0), axis=1, keepdims=True)
    earlier = (owners_col == owners_f) & (row < col) & (row < live)
    rank = jnp.sum(jnp.where(earlier, 1.0, 0.0), axis=0, keepdims=True)
    lane = iota((1, blocks), 1)
    target = jnp.where(lane < live, owners_f * CAP + rank, -1.0)
    pick = jnp.where(iota((slots, blocks), 0).astype(F32) == target, 1.0, 0.0).astype(BF16)
    err = error[...]
    rest = jnp.concatenate(
        [innovation[...] / (err * err), offset[0], offset[1], cell[...].astype(F32)], axis=1
    )
    out = None
    for _ in range(3):
        part = rest.astype(BF16)
        term = jnp.dot(pick, part, preferred_element_type=F32)
        out = term if out is None else out + term
        rest = rest - part.astype(F32)
    for f in range(FIELDS):
        send[pl.ds(f, slots, stride=FIELDS), :] = out[:, f * LANE : (f + 1) * LANE]


def weigh(values, k, rows, cols, index, lhs, rhs):
    amount, north, east = values[0:1], values[1:2], values[2:3]
    cell = values[3:4].astype(jnp.int32)
    cell_row = lax.div(cell, cols)
    cell_col = lax.rem(cell, cols)
    part = lax.rem(cell_col, SPLIT)
    spot = iota((8, LANE), 0)
    across = jnp.where(spot == part, 1.0 - east, jnp.where(spot == part + 1, east, 0.0)) * amount
    down_at = iota((rows, LANE), 0)
    down = jnp.where(down_at == cell_row, 1.0 - north, jnp.where(down_at == cell_row + 1, north, 0.0))
    below = jnp.where(cell_row == rows - 1, north, 0.0) * across
    pieces = [down * across[c : c + 1] for c in range(PART)]
    pieces.append(jnp.concatenate([below, jnp.zeros((8, LANE), F32)], axis=0))
    second = PART * rows + 16
    for c, piece in enumerate(pieces):
        end = c * rows + piece.shape[0]
        main = piece.astype(BF16)
        lhs[k, c * rows : end, :] = main
        lhs[k, second + c * rows : second + end, :] = (piece - main.astype(F32)).astype(BF16)
    spots = index[...]
    column = lax.div(cell_col, SPLIT).astype(F32).astype(BF16)
    rhs[k] = jnp.where(spots == column, jnp.ones_like(spots), jnp.zeros_like(spots))


def weigh_group(recv, start, rows, cols, index, lhs, rhs):
    for i in range(0, GROUP * ROWS, 8):
        pair = recv[pl.ds(pl.multiple_of(start + i, 8), 8), :]
        for k in range(0, 8, FIELDS):
            weigh(pair[k : k + FIELDS], (i + k) // FIELDS, rows, cols, index, lhs, rhs)


def add_group(lhs, rhs, total):
    total[...] += lax.dot_general(
        jnp.concatenate([lhs[k] for k in range(lhs.shape[0])], axis=1),
        jnp.concatenate([rhs[k] for k in range(rhs.shape[0])], axis=1),
        (((1,), (1,)), ((), ())),
        preferred_element_type=F32,
    )


def total_shape(rows, cols):
    return (2 * (PART * rows + 16), cols // SPLIT)


def unpack(total, rows, cols, part):
    wide = cols // SPLIT
    half = rows // 2
    count = PART * rows + 16
    acc = total[0:count, :] + total[count : 2 * count, :]
    under = acc[PART * rows : PART * rows + 8]
    top = iota((8, wide), 0) == 0
    fields = []
    for c in range(PART):
        row = jnp.where(top, jnp.broadcast_to(under[c : c + 1], (8, wide)), 0.0)
        fields.append(jnp.concatenate([acc[c * rows : (c + 1) * rows], row], axis=0))
    carried = pltpu.roll(fields[SPLIT], 1, 1)
    first = iota(carried.shape, 1) == 0
    past = jnp.where(first, carried, 0.0)[:, :LANE]
    fields[0] = fields[0] + jnp.where(first, 0.0, carried)
    size = SPLIT * LANE
    source, place = iota((size, size), 0), iota((size, size), 1)
    order = jnp.where(place == SPLIT * (source % LANE) + source // LANE, 1.0, 0.0).astype(BF16)
    strips = []
    for j in range(wide // LANE):
        rest = jnp.concatenate([f[:, j * LANE : (j + 1) * LANE] for f in fields[:SPLIT]], axis=1)
        out = None
        for _ in range(3):
            piece = rest.astype(BF16)
            term = jnp.dot(piece, order, preferred_element_type=F32)
            out = term if out is None else out + term
            rest = rest - piece.astype(F32)
        strips.append(out)
    for j, out in enumerate(strips):
        at = slice(j * size, (j + 1) * size)
        part[0, 0:half, at] = out[0:half]
        part[0, half : half + 8, at] = jnp.zeros((8, size), F32)
        part[1, :, at] = out[half:]
    part[0, 0:half, cols:] = past[0:half]
    part[0, half : half + 8, cols:] = jnp.zeros((8, LANE), F32)
    part[1, :, cols:] = past[half:]


def add_up(values):
    while len(values) > 1:
        rest = values[len(values) & ~1 :]
        values = [values[i] + values[i + 1] for i in range(0, len(values) - 1, 2)] + rest
    return values[0]


def coefficients(mu):
    start = mu[0]
    mu = [m / start for m in mu]
    gram = {}
    for s in range(2 * ITERS + 1):
        for d in range(s + 1):
            gram[s, d] = 0.5 * (mu[s] + mu[d])

    def inner(a, b):
        terms = [a[i] * b[j] * gram[i + j, abs(i - j)] for i in range(len(a)) for j in range(len(b))]
        return add_up(terms)

    def operate(a):
        out = [CENTRE * v for v in a] + [None]
        for i, v in enumerate(a):
            for j, f in ((1, RADIUS),) if i == 0 else ((i + 1, RADIUS / 2), (i - 1, RADIUS / 2)):
                out[j] = f * v if out[j] is None else out[j] + f * v
        return out

    one = jnp.ones_like(start)
    field, residual, direction = [], [one], [one]
    norm = one
    worst = one
    for _ in range(ITERS):
        applied = operate(direction)
        step = norm / inner(direction, applied)
        field = [
            step * d + (field[i] if i < len(field) else 0.0) for i, d in enumerate(direction)
        ]
        residual = [
            (residual[i] if i < len(residual) else 0.0) - step * a for i, a in enumerate(applied)
        ]
        after = inner(residual, residual)
        size = add_up([jnp.abs(v) for v in residual])
        worst = jnp.maximum(worst, jnp.where(after > 0, size * size / after, 1e30))
        ratio = after / norm
        direction = [
            v + (ratio * direction[i] if i < len(direction) else 0.0) for i, v in enumerate(residual)
        ]
        norm = after
    sound = jnp.where(worst < TRUST, 1.0, 0.0)
    return field, residual, sound


def step_kernel(
    n_lat,
    n_lon,
    innovation,
    error,
    offset,
    cell,
    owner,
    count,
    land,
    inertia,
    depth,
    field_out,
    residual_out,
    forcing_out,
    sound_out,
    send,
    recv,
    lhs_a,
    rhs_a,
    lhs_b,
    rhs_b,
    index,
    total,
    part,
    got,
    mine,
    west,
    east,
    tall,
    above,
    below,
    coef,
    cond,
    basis,
    line_in,
    line_at,
    rank_in,
    rank_at,
    out_sem,
    in_sem,
    send_sem,
    recv_sem,
    line_send,
    line_recv,
    rank_send,
    rank_recv,
):
    rows, cols = land.shape
    high, wide = rows + 2 * EDGE, cols + 2 * LANE
    lat, lon, obs = lax.axis_index("lat"), lax.axis_index("lon"), lax.axis_index("obs")
    tiles = n_lat * n_lon
    ranks = 2 * n_lat
    rank = lat * 2 + obs
    quads = n_lon // GROUP
    groups = n_lat * quads

    def on_line(k):
        return {"lon": k}

    def on_rank(k):
        return {"lat": lax.div(k, 2), "obs": lax.rem(k, 2)}

    def on_tile(k):
        return {"lat": lax.div(k, n_lon), "lon": lax.rem(k, n_lon)}

    me = lat * n_lon + lon
    barrier = pltpu.get_barrier_semaphore()

    def greet_tile(d, carry):
        device = on_tile(lax.rem(me + d, tiles))
        pl.semaphore_signal(barrier, 1, device_id=device, device_id_type=MESH)
        return carry

    def greet_other(d, carry):
        device = {"lat": lax.rem(lat + d, n_lat), "obs": 1 - obs}
        pl.semaphore_signal(barrier, 1, device_id=device, device_id_type=MESH)
        return carry

    lax.fori_loop(1, tiles, greet_tile, 0)
    lax.fori_loop(0, n_lat, greet_other, 0)

    inner_rows, inner_cols = slice(EDGE, EDGE + rows), slice(LANE, LANE + cols)
    coef[0, inner_rows, inner_cols] = land[...].astype(F32) * depth[...]
    coef[1, inner_rows, inner_cols] = inertia[...]
    arrange(tiles, innovation, error, offset, cell, owner, count, send)
    pl.semaphore_wait(barrier, tiles - 1 + n_lat)

    def copy(k, src, dst, device):
        c = pltpu.make_async_remote_copy(
            src_ref=src,
            dst_ref=dst,
            send_sem=send_sem.at[k],
            recv_sem=recv_sem.at[k],
            device_id=device,
            device_id_type=MESH,
        )
        c.start()
        return c

    to_east, to_west = on_line(lax.rem(lon + 1, n_lon)), on_line(lax.rem(lon + n_lon - 1, n_lon))
    to_south, to_north = on_rank(lax.rem(rank + 1, ranks)), on_rank(lax.rem(rank + ranks - 1, ranks))
    own = pl.ds(EDGE, rows)

    coef_e = copy(1, coef.at[:, own, pl.ds(cols, LANE)], coef.at[:, own, pl.ds(0, LANE)], to_east)
    coef_w = copy(2, coef.at[:, own, pl.ds(LANE, LANE)], coef.at[:, own, pl.ds(LANE + cols, LANE)], to_west)

    quad, place = lax.div(lon, GROUP), lax.rem(lon, GROUP)

    def away(t):
        j = lax.div(t, quads)
        odd = lax.rem(j, 2)
        return lax.rem(odd * lax.div(j + 1, 2) + (1 - odd) * (n_lat - lax.div(j, 2)), n_lat)

    def rows_of(k):
        return pl.ds(k * ROWS, ROWS)

    my_group = lat * quads + quad

    def deliver(t, carry):
        to_lat = lax.rem(lat + n_lat - away(t), n_lat)
        to_quad = lax.rem(quad + quads - lax.rem(t, quads), quads)
        for d in range(GROUP):
            to_lon = to_quad * GROUP + lax.rem(place + d, GROUP)
            transfer = pltpu.make_async_remote_copy(
                src_ref=send.at[rows_of(to_lat * n_lon + to_lon), :],
                dst_ref=recv.at[rows_of(me), :],
                send_sem=out_sem,
                recv_sem=in_sem.at[my_group],
                device_id={"lat": to_lat, "lon": to_lon},
                device_id_type=MESH,
            )
            if d:
                transfer.start()
            else:
                pl.when(t > 0)(transfer.start)
        return carry

    pltpu.make_async_copy(send.at[rows_of(me), :], recv.at[rows_of(me), :], in_sem.at[my_group]).start()
    lax.fori_loop(0, min(AHEAD, groups), deliver, 0)
    total[...] = jnp.zeros_like(total)
    index[...] = iota(index.shape, 0).astype(F32).astype(BF16)
    height = GROUP * ROWS

    def group_of(t):
        from_lat = lax.rem(lat + away(t), n_lat)
        return from_lat * quads + lax.rem(quad + lax.rem(t, quads), quads)

    def await_group(t):
        g = group_of(t)
        landed = recv.at[pl.ds(pl.multiple_of(g * height, 8), height), :]
        pltpu.make_async_copy(landed, landed, in_sem.at[g]).wait()

    def weigh_next(t, lhs, rhs):
        weigh_group(recv, group_of(t) * height, 2 * rows, cols, index, lhs, rhs)

    await_group(0)
    weigh_next(0, lhs_a, rhs_a)

    def spread_two(i, carry):
        begin = jnp.minimum(2 * i + AHEAD, groups)
        lax.fori_loop(begin, jnp.minimum(begin + 2, groups), deliver, 0)
        await_group(2 * i + 1)
        add_group(lhs_a, rhs_a, total)
        weigh_next(2 * i + 1, lhs_b, rhs_b)
        await_group(2 * i + 2)
        add_group(lhs_b, rhs_b, total)
        weigh_next(2 * i + 2, lhs_a, rhs_a)
        return carry

    lax.fori_loop(0, groups // 2 - 1, spread_two, 0)
    await_group(groups - 1)
    weigh_next(groups - 1, lhs_b, rhs_b)
    add_group(lhs_a, rhs_a, total)
    add_group(lhs_b, rhs_b, total)
    gone = send.at[pl.ds(0, (tiles - 1) * ROWS), :]
    pltpu.make_async_copy(gone, gone, out_sem).wait()
    unpack(total, 2 * rows, cols, part)

    coef_e.wait_recv()
    coef_w.wait_recv()
    coef_s = copy(5, coef.at[:, pl.ds(rows, EDGE), :], coef.at[:, pl.ds(0, EDGE), :], to_south)
    coef_n = copy(6, coef.at[:, pl.ds(EDGE, EDGE), :], coef.at[:, pl.ds(EDGE + rows, EDGE), :], to_north)
    pair = copy(0, part.at[1 - obs], got, {"obs": 1 - obs})
    pair.wait_recv()
    mine[...] = part[obs] + got[...]
    mine_e = copy(3, mine.at[:, pl.ds(cols - LANE, 2 * LANE)], west, to_east)
    mine_w = copy(4, mine.at[:, pl.ds(0, LANE)], east, to_west)
    mine_e.wait_recv()
    mine_w.wait_recv()
    tall[:, 0:LANE] = west[:, 0:LANE]
    tall[:, LANE : 2 * LANE] = mine[:, 0:LANE] + west[:, LANE:]
    tall[:, 2 * LANE : LANE + cols] = mine[:, LANE:cols]
    tall[:, LANE + cols :] = mine[:, cols:] + east[...]
    tall_s = copy(7, tall.at[pl.ds(rows - EDGE, 2 * EDGE), :], above, to_south)
    tall_n = copy(8, tall.at[pl.ds(0, EDGE), :], below, to_north)
    coef_s.wait_recv()
    coef_n.wait_recv()
    conduct = coef[0]
    north = jnp.sqrt(conduct * pltpu.roll(conduct, 1, 0))
    south = pltpu.roll(north, high - 1, 0)
    left = jnp.sqrt(conduct * pltpu.roll(conduct, 1, 1))
    right = pltpu.roll(left, wide - 1, 1)
    cond[0] = (coef[1] + north + south + left + right - CENTRE) * (1.0 / RADIUS)
    cond[1] = north * (1.0 / RADIUS)
    cond[2] = south * (1.0 / RADIUS)
    cond[3] = left * (1.0 / RADIUS)
    cond[4] = right * (1.0 / RADIUS)
    tall_s.wait_recv()
    tall_n.wait_recv()
    ocean = coef[0] > 0
    raw = jnp.concatenate(
        [
            above[0:EDGE, :],
            tall[0:EDGE, :] + above[EDGE:, :],
            tall[EDGE:rows, :],
            below[...] + tall[rows:, :],
        ],
        axis=0,
    )
    basis[0] = jnp.where(ocean, raw, 0.0)
    forcing_out[...] = basis[0, inner_rows, inner_cols]

    def operate(v):
        return (
            cond[0] * v
            - cond[1] * pltpu.roll(v, 1, 0)
            - cond[2] * pltpu.roll(v, high - 1, 0)
            - cond[3] * pltpu.roll(v, 1, 1)
            - cond[4] * pltpu.roll(v, wide - 1, 1)
        )

    for k in range(ITERS):
        after = operate(basis[k])
        basis[k + 1] = after if k == 0 else 2.0 * after - basis[k - 1]

    def dot(i, j):
        pieces = []
        for a in range(EDGE, EDGE + rows, 8):
            for b in range(LANE, LANE + cols, LANE):
                pieces.append(basis[i, a : a + 8, b : b + LANE] * basis[j, a : a + 8, b : b + LANE])
        return jnp.sum(add_up(pieces), axis=0, keepdims=True)

    pairs = [(k // 2, (k + 1) // 2) for k in range(2 * ITERS + 1)]
    sums = [dot(i, j) for i, j in pairs]
    stack = jnp.concatenate(sums + [jnp.zeros((16 - len(sums), LANE), F32)], axis=0)
    column = jnp.sum(stack, axis=1, keepdims=True)
    diag = iota((16, LANE), 0) == iota((16, LANE), 1)
    line_in[...] = jnp.sum(jnp.where(diag, column, 0.0), axis=0, keepdims=True)

    def share(count, me, device, value, at, s_sem, r_sem):
        def copy_of(slot, k, target):
            return pltpu.make_async_remote_copy(
                src_ref=value,
                dst_ref=at.at[slot],
                send_sem=s_sem.at[k],
                recv_sem=r_sem.at[slot],
                device_id=device(target),
                device_id_type=MESH,
            )

        half = count // 2
        offsets = [half] + [half + s * k for k in range(1, half) for s in (1, -1)]
        for d in offsets:
            copy_of(me, d, lax.rem(me + d, count)).start()
        at[me] = value[...]
        for d in reversed(offsets):
            copy_of(lax.rem(me + count - d, count), d, lax.rem(me + d, count)).wait_recv()
        for d in offsets:
            copy_of(me, d, lax.rem(me + d, count)).wait_send()
        return add_up([at[k] for k in range(count)])

    rank_in[...] = share(n_lon, lon, on_line, line_in, line_at, line_send, line_recv)
    sums = share(ranks, rank, on_rank, rank_in, rank_at, rank_send, rank_recv)
    lane = iota((1, LANE), 1)
    raw_sums = [
        jnp.sum(jnp.where(lane == k, sums, 0.0), axis=1, keepdims=True) for k in range(2 * ITERS + 1)
    ]
    mu = [
        raw_sums[k] if k < 2 else 2.0 * raw_sums[k] - raw_sums[k % 2] for k in range(2 * ITERS + 1)
    ]
    field, residual, sound = coefficients(mu)
    views = [basis[k, inner_rows, inner_cols] for k in range(ITERS + 1)]
    field_out[...] = add_up([c * v for c, v in zip(field, views)])
    residual_out[...] = add_up([c * v for c, v in zip(residual, views)])
    sound_out[...] = jnp.broadcast_to(sound, (1, LANE))
    for c in (pair, coef_e, coef_w, mine_e, mine_w, coef_s, coef_n, tall_s, tall_n):
        c.wait_send()


def step(n_lat, n_lon, innovation, error, offset, cell, owner, count, land, inertia, depth):
    rows, cols = land.shape
    high, wide = rows + 2 * EDGE, cols + 2 * LANE
    own = jax.ShapeDtypeStruct((rows, cols), F32)
    vmem = pl.BlockSpec(memory_space=pltpu.VMEM)
    ranks = 2 * n_lat
    tiles = n_lat * n_lon
    groups = tiles // GROUP
    tall = total_shape(2 * rows, cols)
    deep = GROUP * CAP
    return pl.pallas_call(
        functools.partial(step_kernel, n_lat, n_lon),
        out_shape=(own, own, own, jax.ShapeDtypeStruct((1, LANE), F32)),
        in_specs=[vmem] * 5 + [pl.BlockSpec(memory_space=pltpu.SMEM)] + [vmem] * 3,
        out_specs=(vmem,) * 4,
        scratch_shapes=[
            pltpu.VMEM((tiles * ROWS, LANE), F32),
            pltpu.VMEM((tiles * ROWS, LANE), F32),
            pltpu.VMEM((deep, tall[0], LANE), BF16),
            pltpu.VMEM((deep, tall[1], LANE), BF16),
            pltpu.VMEM((deep, tall[0], LANE), BF16),
            pltpu.VMEM((deep, tall[1], LANE), BF16),
            pltpu.VMEM((tall[1], LANE), BF16),
            pltpu.VMEM(tall, F32),
            pltpu.VMEM((2, rows + EDGE, cols + LANE), F32),
            pltpu.VMEM((rows + EDGE, cols + LANE), F32),
            pltpu.VMEM((rows + EDGE, cols + LANE), F32),
            pltpu.VMEM((rows + EDGE, 2 * LANE), F32),
            pltpu.VMEM((rows + EDGE, LANE), F32),
            pltpu.VMEM((rows + EDGE, wide), F32),
            pltpu.VMEM((2 * EDGE, wide), F32),
            pltpu.VMEM((EDGE, wide), F32),
            pltpu.VMEM((2, high, wide), F32),
            pltpu.VMEM((5, high, wide), F32),
            pltpu.VMEM((ITERS + 1, high, wide), F32),
            pltpu.VMEM((1, LANE), F32),
            pltpu.VMEM((n_lon, 1, LANE), F32),
            pltpu.VMEM((1, LANE), F32),
            pltpu.VMEM((ranks, 1, LANE), F32),
            pltpu.SemaphoreType.DMA,
            pltpu.SemaphoreType.DMA((groups,)),
            pltpu.SemaphoreType.DMA((9,)),
            pltpu.SemaphoreType.DMA((9,)),
            pltpu.SemaphoreType.DMA((n_lon,)),
            pltpu.SemaphoreType.DMA((n_lon,)),
            pltpu.SemaphoreType.DMA((ranks,)),
            pltpu.SemaphoreType.DMA((ranks,)),
        ],
        compiler_params=pltpu.CompilerParams(collective_id=1, has_side_effects=True),
    )(innovation, error, offset, cell, owner, count, land, inertia, depth)


def shifted(value, axis, steps):
    count = lax.axis_size(axis)
    return lax.ppermute(value, axis, [(i, (i + steps) % count) for i in range(count)])


def border(block):
    for axis, dim in ((("lat", "obs"), 0), ("lon", 1)):
        size = block.shape[dim]
        low = shifted(lax.slice_in_dim(block, size - 1, size, axis=dim), axis, 1)
        high = shifted(lax.slice_in_dim(block, 0, 1, axis=dim), axis, -1)
        block = jnp.concatenate([low, block, high], axis=dim)
    return block


def stepwise(sound, field, residual, forcing, land, own, sea):
    def whole(value):
        return lax.psum(jnp.sum(value), ("lat", "lon", "obs"))

    def step(_, state):
        (field, residual, direction, before), depth, inertia = lax.optimization_barrier(
            (state, sea, own)
        )
        conduct = land.astype(F32) * depth
        padded = border(conduct)
        north = jnp.sqrt(conduct * padded[:-2, 1:-1])
        south = jnp.sqrt(conduct * padded[2:, 1:-1])
        west = jnp.sqrt(conduct * padded[1:-1, :-2])
        east = jnp.sqrt(conduct * padded[1:-1, 2:])
        diagonal = inertia + north + south + west + east
        norm = whole(residual * residual)
        direction = residual + norm / before * direction
        outer = border(direction)
        applied = (
            diagonal * direction
            - north * outer[:-2, 1:-1]
            - south * outer[2:, 1:-1]
            - west * outer[1:-1, :-2]
            - east * outer[1:-1, 2:]
        )
        size = norm / whole(direction * applied)
        return field + size * direction, residual - size * applied, direction, norm

    state = (
        jnp.where(sound, field, 0.0),
        jnp.where(sound, residual, forcing),
        jnp.zeros_like(forcing),
        jnp.float32(1.0),
    )
    return lax.fori_loop(0, jnp.where(sound, 0, ITERS), step, state)[:2]


def body(n_lat, n_lon, *inputs):
    land, inertia, depth = inputs[-3:]
    field, residual, forcing, sound = step(n_lat, n_lon, *inputs)
    return stepwise(sound[0, 0] > 0.5, field, residual, forcing, land, inertia, depth)


def solution(mesh):
    split = ("lat", "lon", "obs")
    grid = P(("lat", "obs"), "lon")
    return jax.shard_map(
        functools.partial(body, mesh.shape["lat"], mesh.shape["lon"]),
        mesh=mesh,
        in_specs=(
            P(split, None),
            P(split, None),
            P(None, split, None),
            P(split, None),
            P(split, None),
            P(split),
            grid,
            grid,
            grid,
        ),
        out_specs=(grid, grid),
        check_vma=False,
    )
```
